32 devices in a mesh: groups: 2 (over y), seq: 4 (over z), batch: 4 (over x, core).
Axes of the slice: x: 2, y: 2, z: 4, core: 2. Of those that a mesh axis runs over, the one named last changes fastest.
Arguments:
- queries: bfloat16 [8, 512, 2048], P(('groups', 'batch'), 'seq'), parts along dimension 0, may hold values from -80 to 80, as said below
- keys: bfloat16 [8, 512, 512], P(('groups', 'batch'), 'seq'), parts along dimension 0, may hold values from -4.5 to 4.5
- values: bfloat16 [8, 512, 512], P(('groups', 'batch'), 'seq'), parts along dimension 0, may hold values from -6 to 6
Outputs:
- attended: bfloat16 [8, 512, 2048], P(('groups', 'batch'), 'seq'), parts along dimension 0
The draws below stay inside these ranges and needn't reach their ends.
There are 2 independent parts, one for each index of `groups`. The reference program is written for one: setup_inputs(seed, part) draws one part's arguments, and reference() takes and returns one part's arrays. A program takes and returns all parts, laid end to end along the dimension named above; each array names one. Nothing has to cross between parts.
Inputs may be any that keep to these rules, and one draw needn't show every extreme that they name: `queries`: query vectors of order a few units; a few positions may hold much larger entries.
All inputs are finite; a program needn't handle non-finite values.
Results may differ from the reference program's by a relative error of at most 0.009.
Values may be sent and summed in bfloat16 or wider, within the bound.
A program may use at most 64 MiB of HBM per device.

```python
import math
import jax
import jax.numpy as jnp
from jax import lax

QUERY_HEADS = 16
KEY_VALUE_HEADS = 4
HEAD_SIZE = 128
SEQUENCE_LENGTH = 512
GROUP_SEQUENCES = 4


def plant_plan(key):
    start_offset = jnp.clip(jax.random.normal(jax.random.fold_in(key, 1), (GROUP_SEQUENCES, SEQUENCE_LENGTH, KEY_VALUE_HEADS * HEAD_SIZE), jnp.float32), -4.5, 4.5)
    return start_offset


def draw_keys(key, part):
    start_offset = plant_plan(key)
    return start_offset.astype(jnp.bfloat16)


def draw_queries(key, part):
    return jnp.clip(2.0 * jax.random.normal(jax.random.fold_in(key, 5), (GROUP_SEQUENCES, SEQUENCE_LENGTH, QUERY_HEADS * HEAD_SIZE), jnp.float32), -12.0, 12.0).astype(jnp.bfloat16)


def block_levels(key, extent, pieces, low, top_value):
    factor_of, own = 1.0, jax.random.fold_in(key, 6)
    for axis_at, parts in pieces:
        draws = jnp.exp(jax.random.uniform(jax.random.fold_in(own, axis_at), (parts,), jnp.float32, low / len(pieces), top_value / len(pieces)))
        factor_of = factor_of * jnp.repeat(draws, extent[axis_at] // parts).reshape([-1 if axis == axis_at else 1 for axis in range(len(extent))])
    return factor_of


def scatter_about(stream_key, dims, scale, reach, shards=(), kind=jnp.bfloat16):
    gain = block_levels(stream_key, dims, shards, -0.22, 0.18) if shards else 1.0
    drawn = jax.random.normal(stream_key, dims, jnp.float32) * scale * gain
    return jnp.minimum(jnp.maximum(drawn, -reach), reach).astype(kind)


def setup_inputs(seed: int = 0, part: int = 0) -> dict:
    seeds = jax.random.split(jax.random.key(seed), 4)
    own_keys = jax.random.split(jax.random.fold_in(seeds[3], part), 4)
    queries = draw_queries(jax.random.fold_in(jax.random.fold_in(seeds[3], part), 71), part)
    keys = draw_keys(jax.random.fold_in(jax.random.fold_in(seeds[3], part), 71), part)
    values = scatter_about(own_keys[2], (GROUP_SEQUENCES, SEQUENCE_LENGTH, KEY_VALUE_HEADS * HEAD_SIZE), 1.0, 6.0, ((0, 4), (1, 4)))
    return {"queries": queries, "keys": keys, "values": values}


def attend_block(rows_of_query, start, keys_single_float, values_single_float):
    rows_per_block = rows_of_query.shape[0]
    query_heads_per_group = QUERY_HEADS // KEY_VALUE_HEADS
    query_single_float = rows_of_query.astype(jnp.float32).reshape(rows_per_block, KEY_VALUE_HEADS, query_heads_per_group, HEAD_SIZE)
    scores = jnp.einsum('qkgd,pkd->qkgp', query_single_float, keys_single_float) / math.sqrt(HEAD_SIZE)
    row_pos = start + jnp.arange(rows_per_block, dtype=jnp.int32)
    key_pos = jnp.arange(SEQUENCE_LENGTH, dtype=jnp.int32)
    visible = (key_pos[None, :] <= row_pos[:, None])[:, None, None, :]
    scores = jnp.where(visible, scores, -jnp.inf)
    weights = jax.nn.softmax(scores, axis=-1).astype(jnp.bfloat16)
    mixed = jnp.einsum('qkgp,pkd->qkgd', weights.astype(jnp.float32), values_single_float)
    return mixed.reshape(rows_per_block, QUERY_HEADS * HEAD_SIZE).astype(jnp.bfloat16)

def one_sequence(operands):
    seq_queries, sequence_keys, sequence_values = operands
    keys_single_float = sequence_keys.astype(jnp.float32).reshape(SEQUENCE_LENGTH, KEY_VALUE_HEADS, HEAD_SIZE)
    values_single_float = sequence_values.astype(jnp.float32).reshape(SEQUENCE_LENGTH, KEY_VALUE_HEADS, HEAD_SIZE)
    rows_per_block = min(512, SEQUENCE_LENGTH)
    num_blocks = SEQUENCE_LENGTH // rows_per_block
    query_blocks = seq_queries.reshape(num_blocks, rows_per_block, QUERY_HEADS * HEAD_SIZE)
    starts = jnp.arange(num_blocks, dtype=jnp.int32) * rows_per_block

    def visit_block(block_args):
        return attend_block(block_args[0], block_args[1], keys_single_float, values_single_float)
    outputs = lax.map(visit_block, (query_blocks, starts))
    return outputs.reshape(SEQUENCE_LENGTH, QUERY_HEADS * HEAD_SIZE)

def reference(queries, keys, values):
    return lax.map(one_sequence, (queries, keys, values))
```

```python
import functools
import math

import jax
import jax.numpy as jnp
from jax import lax
from jax.experimental import pallas as pl
from jax.experimental.pallas import tpu as pltpu
from jax.sharding import PartitionSpec as P

HEAD_SIZE = 128
SCALE = math.log2(math.e) / math.sqrt(HEAD_SIZE)
MESH = pl.DeviceIdType.MESH

SCHEDULED = 4

FIRST, NEXT, MERGE = range(3)
KEEP, FINISH, RETURN = range(3)
CODE = 2**14


def pack(op, slot, g, answer=0, wait=0, forward=0, then=0, flag=KEEP):
    code = 0
    for value, size in ((flag, 4), (then, 8), (forward, 2), (wait, 2), (answer, 2), (g, 4), (slot, 4), (op, 4)):
        code = code * size + value
    return code


def moved_heads(n, groups, phase):
    return 0 if n < 4 else groups // (2 if phase == 0 else 4)


def order_of(top, groups, moved, phase):
    stay = list(range(moved, groups))
    older = range(top - 1, -1, -1)
    if phase == 0 and moved:
        out = [(top, 0)] + [(top, g) for g in stay] + [(b, 0) for b in older]
        for g in range(1, moved):
            out += [(b, g) for b in range(top, -1, -1)]
        return out + [(b, g) for b in older for g in stay]
    ahead = [(top, g) for g in stay[1:]]
    out = [(top, stay[0])]
    behind = [(b, g) for b in older for g in stay[1:] + stay[:1]]
    for i, unit in enumerate(behind):
        out += [unit] + (ahead[i - 1 : i] if 0 < i else [])
    out += ahead[max(len(behind) - 1, 0) :]
    for g in range(moved):
        out += [(b, g) for b in [*older, top]]
    return out


def script(n, groups, phase, rank):
    moved = moved_heads(n, groups, phase)
    helper, last = n - 2, n - 1
    order = order_of(max(n - 3, 0), groups, moved, phase)

    def sends(r):
        mine = [(b, g) for b, g in order if b <= r]
        if r < helper:
            return mine
        own = [(r, g) for g in range(moved, groups)]
        return own + [(b, g) for b, g in mine if g >= moved]

    queue = sends(rank) if rank < last else []
    arrivals = sends(helper) if rank == last else [(b, g) for b, g in order if b < rank]
    before = []
    while queue and queue[0][0] == rank:
        before.append(queue.pop(0)[1])

    steps = []
    left = {g: rank for g in range(groups)}
    waiting = {g: rank for g in range(moved)} if rank == helper else {}
    seen = {g: [] for g in waiting}
    ready = set()
    returned = 0

    def start_answer(g):
        ready.add(g)
        steps.append(pack(FIRST, 0, g, answer=1))
        for slot in seen[g]:
            steps.append(pack(NEXT, slot, g, answer=1))

    for i, (b, g) in enumerate(arrivals):
        slot = rank - b
        how = dict(wait=1)
        if queue and queue[0] == (b, g):
            queue.pop(0)
            how["forward"] = 1
            if queue and queue[0][0] == rank:
                how["then"] = queue.pop(0)[1] + 1
        left[g] -= 1
        if g in waiting:
            waiting[g] -= 1
            if g in ready:
                steps.append(pack(NEXT, slot, g, answer=1, flag=KEEP if waiting[g] else RETURN, **how))
                how = {}
            seen[g].append(slot)
        ends = left[g] == 0 and not (rank == last and g < moved)
        steps.append(pack(NEXT, slot, g, flag=FINISH if ends else KEEP, **how))
        if i + 1 < len(arrivals):
            h = arrivals[i + 1][1]
            if h in waiting and waiting[h] == 1:
                start_answer(h)
        if rank == last:
            while returned < moved and returns_before(order, moved, returned, groups) <= i + 1:
                steps.append(pack(MERGE, 0, returned))
                returned += 1
    if rank == last:
        steps += [pack(MERGE, 0, g) for g in range(returned, moved)]
    assert not queue
    return before, steps


def returns_before(order, moved, g, groups):
    at = max(i for i, (_, h) in enumerate(order) if h == g)
    return groups - moved + sum(1 for _, h in order[:at] if h >= moved)


def scheduled_kernel(
    n, groups, per_group, most,
    q_hbm, k_hbm, v_hbm, o,
    q, kv, m, acc, back, back_stats, mine, mine_stats,
    load_sem, q_sem, send_sem, recv_sem, ask_send, ask_recv, back_send, back_recv,
):
    rows = kv.shape[2] // 2
    tall = per_group * rows
    me = lax.axis_index("seq")
    phase = lax.rem(lax.axis_index("batch"), 2)
    last, helper = n - 1, n - 2

    def kv_load(g):
        cols = pl.ds(g * HEAD_SIZE, HEAD_SIZE)
        return (
            pltpu.make_async_copy(
                k_hbm.at[0, :, cols], kv.at[0, g, pl.ds(0, rows)], load_sem.at[0, g]
            ),
            pltpu.make_async_copy(
                v_hbm.at[0, :, cols], kv.at[0, g, pl.ds(rows, rows)], load_sem.at[1, g]
            ),
        )

    def q_load(g, h):
        return pltpu.make_async_copy(
            q_hbm.at[0, :, pl.ds((g * per_group + h) * HEAD_SIZE, HEAD_SIZE)],
            q.at[g, pl.ds(h * rows, rows)],
            q_sem.at[g, h],
        )

    def send(slot, g):
        return pltpu.make_async_remote_copy(
            src_ref=kv.at[slot, g],
            dst_ref=kv.at[slot + 1, g],
            send_sem=send_sem.at[slot, g],
            recv_sem=recv_sem.at[slot + 1, g],
            device_id={"seq": jnp.minimum(me + 1, last)},
            device_id_type=MESH,
        )

    def receive(slot, g):
        return pltpu.make_async_remote_copy(
            src_ref=kv.at[slot, g],
            dst_ref=kv.at[slot, g],
            send_sem=send_sem.at[slot, g],
            recv_sem=recv_sem.at[slot, g],
            device_id={"seq": jnp.minimum(me + 1, last)},
            device_id_type=MESH,
        )

    def ask(g):
        return pltpu.make_async_remote_copy(
            src_ref=q.at[g],
            dst_ref=q.at[groups + g],
            send_sem=ask_send.at[g],
            recv_sem=ask_recv.at[g],
            device_id={"seq": jnp.int32(helper)},
            device_id_type=MESH,
        )

    def give(g):
        return (
            pltpu.make_async_remote_copy(
                src_ref=mine.at[g],
                dst_ref=back.at[g],
                send_sem=back_send.at[0, g],
                recv_sem=back_recv.at[0, g],
                device_id={"seq": jnp.int32(last)},
                device_id_type=MESH,
            ),
            pltpu.make_async_remote_copy(
                src_ref=mine_stats.at[g],
                dst_ref=back_stats.at[g],
                send_sem=back_send.at[1, g],
                recv_sem=back_recv.at[1, g],
                device_id={"seq": jnp.int32(last)},
                device_id_type=MESH,
            ),
        )

    barrier = pltpu.get_barrier_semaphore()

    @pl.when(me > 0)
    def _():
        pl.semaphore_signal(barrier, inc=1, device_id={"seq": me - 1}, device_id_type=MESH)

    if most:
        @pl.when(me == helper)
        def _():
            pl.semaphore_signal(barrier, inc=1, device_id={"seq": jnp.int32(last)}, device_id_type=MESH)

    for g in range(groups):
        for copy in kv_load(g):
            copy.start()
    for g in range(groups):
        for h in range(per_group):
            q_load(g, h).start()

    scripts = {(r, p): script(n, groups, p, r) for r in range(n) for p in range(2)}
    here = {key: (me == key[0]) & (phase == key[1]) for key in scripts}

    def pick(values):
        out = jnp.int32(0)
        for key, value in values.items():
            if value:
                out = jnp.where(here[key], jnp.int32(value), out)
        return out

    count = pick({key: len(steps) for key, (_, steps) in scripts.items()})
    longest = max(len(steps) for _, steps in scripts.values())
    words = []
    for at in range(0, longest, 2):
        pairs = {key: (steps[at : at + 2] + [0, 0])[:2] for key, (_, steps) in scripts.items()}
        words.append(pick({key: low + CODE * high for key, (low, high) in pairs.items()}))

    @pl.when(me < last if not most else me >= 0)
    def _():
        pl.semaphore_wait(barrier, 1)

    for key, (before, _) in scripts.items():
        rank, p = key

        @pl.when(here[key])
        def _(rank=rank, p=p, before=before):
            if rank == last:
                for g in range(moved_heads(n, groups, p)):
                    for h in range(per_group):
                        q_load(g, h).wait()
                    ask(g).start()
            for g in before:
                for copy in kv_load(g):
                    copy.wait()
                send(0, g).start()
            for g in range(groups):
                if g not in before:
                    for copy in kv_load(g):
                        copy.wait()
            for g in range(groups):
                if rank < last or g >= moved_heads(n, groups, p):
                    for h in range(per_group):
                        q_load(g, h).wait()

    def scores_of(slot, g, qi):
        return lax.dot_general(
            q[qi],
            kv[slot, g, :rows, :],
            (((1,), (1,)), ((), ())),
            preferred_element_type=jnp.float32,
        )

    def weighted(p, slot, g):
        block = jnp.concatenate(
            [kv[slot, g, rows:, :], jnp.ones((rows, HEAD_SIZE), jnp.bfloat16)], axis=1
        )
        return jnp.dot(p.astype(jnp.bfloat16), block, preferred_element_type=jnp.float32)

    def write(total, g):
        done = (total[:, :HEAD_SIZE] / total[:, HEAD_SIZE:]).astype(jnp.bfloat16)
        for h in range(per_group):
            at = pl.multiple_of((g * per_group + h) * HEAD_SIZE, HEAD_SIZE)
            o[0, :, pl.ds(at, HEAD_SIZE)] = done[h * rows : (h + 1) * rows]

    def conclude(qi, g, flag):
        @pl.when(flag == FINISH)
        def _():
            write(acc[qi], g)

        if most:
            @pl.when(flag == RETURN)
            def _():
                total = acc[qi]
                mine[g] = (total[:, :HEAD_SIZE] / total[:, HEAD_SIZE:]).astype(jnp.bfloat16)
                lane = lax.broadcasted_iota(jnp.int32, (rows, HEAD_SIZE), 1)
                stats = jnp.zeros((rows, HEAD_SIZE), jnp.float32)
                for h in range(per_group):
                    part = pl.ds(h * rows, rows)
                    stats = jnp.where(lane == h, m[qi, part, :], stats)
                    stats = jnp.where(lane == per_group + h, acc[qi, part, HEAD_SIZE:], stats)
                mine_stats[g] = stats.T[: mine_stats.shape[1]]
                for copy in give(g):
                    copy.start()

    row = lax.rem(lax.broadcasted_iota(jnp.int32, (tall, rows), 0), rows)
    column = lax.broadcasted_iota(jnp.int32, (tall, rows), 1)

    @pl.loop(0, groups + count)
    def _(i):
        at = jnp.maximum(i - groups, 0)
        word = words[0] if words else jnp.int32(0)
        for j, other in enumerate(words[1:]):
            word = jnp.where(at >= 2 * (j + 1), other, word)
        code = jnp.where(lax.rem(at, 2) == 0, lax.rem(word, CODE), lax.div(word, CODE))
        own = pack(FIRST, 0, 0) + jnp.where(me == 0, pack(FIRST, 0, 0, flag=FINISH), 0) + pack(FIRST, 0, 1) * i
        code = jnp.where(i < groups, own, code)
        op = lax.rem(code, 4)
        slot = lax.rem(lax.div(code, 4), 4)
        g = lax.rem(lax.div(code, 16), 4)
        answer = lax.rem(lax.div(code, 64), 2)
        wait = lax.rem(lax.div(code, 128), 2)
        forward = lax.rem(lax.div(code, 256), 2)
        then = lax.rem(lax.div(code, 512), 8)
        flag = lax.div(code, 4096)
        qi = g + groups * answer

        @pl.when(wait == 1)
        def _():
            receive(slot, g).wait_recv()

            @pl.when(forward == 1)
            def _():
                send(slot, g).start()

            @pl.when(then > 0)
            def _():
                send(0, then - 1).start()

        if most:
            @pl.when((op == FIRST) & (answer == 1))
            def _():
                ask(g).wait_recv()

        @pl.when(op == FIRST)
        def _():
            ahead = rows * answer
            s = jnp.where(column <= row + ahead, scores_of(0, g, qi), -1e30)
            new_m = jnp.max(s, axis=1, keepdims=True)
            acc[qi] = weighted(jnp.exp2((s - new_m) * SCALE), 0, g)
            m[qi] = jnp.broadcast_to(new_m, m.shape[1:])
            conclude(qi, g, flag)

        @pl.when(op == NEXT)
        def _():
            s = scores_of(slot, g, qi)
            old_m = m[qi]
            new_m = jnp.maximum(old_m, jnp.max(s, axis=1, keepdims=True))
            fade = jnp.exp2((old_m - new_m) * SCALE)
            p = jnp.exp2((s - new_m[:, :1]) * SCALE)
            acc[qi] = acc[qi] * jnp.concatenate([fade, fade], axis=1) + weighted(p, slot, g)
            m[qi] = new_m
            conclude(qi, g, flag)

        if most:
            @pl.when(op == MERGE)
            def _():
                for copy in give(g):
                    copy.wait_recv()
                few = back_stats.shape[1]
                stats = jnp.concatenate(
                    [back_stats[g], jnp.zeros((HEAD_SIZE - few, rows), jnp.float32)], axis=0
                ).T
                for h in range(per_group):
                    part = pl.ds(h * rows, rows)
                    there = stats[:, h : h + 1]
                    here = m[g, part, :]
                    new_m = jnp.maximum(here, there)
                    fade = jnp.exp2((here - new_m) * SCALE)
                    weight = jnp.exp2((there - new_m) * SCALE) * stats[:, per_group + h : per_group + h + 1]
                    top = acc[g, part, :HEAD_SIZE] * fade + back[g, part, :].astype(jnp.float32) * weight
                    low = acc[g, part, HEAD_SIZE:] * fade + weight
                    at = pl.multiple_of((g * per_group + h) * HEAD_SIZE, HEAD_SIZE)
                    o[0, :, pl.ds(at, HEAD_SIZE)] = (top / low).astype(jnp.bfloat16)

    for p in range(2):
        away = moved_heads(n, groups, p)

        @pl.when((me < last) & (phase == p))
        def _(away=away):
            @pl.loop(0, me + 1)
            def _(slot):
                for g in range(groups):
                    if g < away:
                        @pl.when(me < helper)
                        def _():
                            send(slot, g).wait_send()
                    else:
                        send(slot, g).wait_send()

        for g in range(away):
            @pl.when((me == last) & (phase == p))
            def _(g=g):
                ask(g).wait_send()

            @pl.when((me == helper) & (phase == p))
            def _(g=g):
                for copy in give(g):
                    copy.wait_send()


def scheduled(n, queries, keys, values):
    rows, query_width = queries.shape[1:]
    groups = keys.shape[2] // HEAD_SIZE
    per_group = query_width // HEAD_SIZE // groups
    tall = per_group * rows
    most = max(moved_heads(n, groups, p) for p in range(2))
    held = max(most, 1)
    few = -(-2 * per_group // 8) * 8
    hbm = pl.BlockSpec(memory_space=pltpu.HBM)
    total = groups + most
    bytes_held = (
        2 * rows * query_width * 2
        + total * tall * HEAD_SIZE * (2 + 4 + 8)
        + 2 * n * rows * keys.shape[2] * 2
        + 2 * held * (tall * HEAD_SIZE * 2 + few * rows * 4)
    )
    return pl.pallas_call(
        functools.partial(scheduled_kernel, n, groups, per_group, most),
        out_shape=jax.ShapeDtypeStruct(queries.shape, queries.dtype),
        in_specs=[hbm, hbm, hbm],
        out_specs=pl.BlockSpec(memory_space=pltpu.VMEM),
        scratch_shapes=[
            pltpu.VMEM((total, tall, HEAD_SIZE), jnp.bfloat16),
            pltpu.VMEM((n, groups, 2 * rows, HEAD_SIZE), jnp.bfloat16),
            pltpu.VMEM((total, tall, HEAD_SIZE), jnp.float32),
            pltpu.VMEM((total, tall, 2 * HEAD_SIZE), jnp.float32),
            pltpu.VMEM((held, tall, HEAD_SIZE), jnp.bfloat16),
            pltpu.VMEM((held, few, rows), jnp.float32),
            pltpu.VMEM((held, tall, HEAD_SIZE), jnp.bfloat16),
            pltpu.VMEM((held, few, rows), jnp.float32),
            pltpu.SemaphoreType.DMA((2, groups)),
            pltpu.SemaphoreType.DMA((groups, per_group)),
            pltpu.SemaphoreType.DMA((n, groups)),
            pltpu.SemaphoreType.DMA((n, groups)),
            pltpu.SemaphoreType.DMA((held,)),
            pltpu.SemaphoreType.DMA((held,)),
            pltpu.SemaphoreType.DMA((2, held)),
            pltpu.SemaphoreType.DMA((2, held)),
        ],
        compiler_params=pltpu.CompilerParams(
            collective_id=0, has_side_effects=True, vmem_limit_bytes=bytes_held + 4 * 2**20
        ),
    )(*(pltpu.with_memory_space_constraint(x, pltpu.HBM) for x in (queries, keys, values)))


def kernel(
    n, groups, per_group,
    q_hbm, k_hbm, v_hbm, o,
    q, kv, m, acc,
    load_sem, q_sem, send_sem, recv_sem,
):
    rows = q.shape[0]
    me = lax.axis_index("seq")
    right, left = lax.rem(me + 1, n), lax.rem(me + n - 1, n)

    def loads(g):
        cols = pl.ds(g * HEAD_SIZE, HEAD_SIZE)
        return (
            pltpu.make_async_copy(
                k_hbm.at[0, :, cols], kv.at[0, g, pl.ds(0, rows)], load_sem.at[0, g]
            ),
            pltpu.make_async_copy(
                v_hbm.at[0, :, cols], kv.at[0, g, pl.ds(rows, rows)], load_sem.at[1, g]
            ),
        )

    def send(slot, g):
        return pltpu.make_async_remote_copy(
            src_ref=kv.at[slot, g],
            dst_ref=kv.at[slot + 1, g],
            send_sem=send_sem.at[slot, g],
            recv_sem=recv_sem.at[slot + 1, g],
            device_id={"seq": right},
            device_id_type=MESH,
        )

    def receive(slot, g):
        return pltpu.make_async_remote_copy(
            src_ref=kv.at[slot, g],
            dst_ref=kv.at[slot, g],
            send_sem=send_sem.at[slot, g],
            recv_sem=recv_sem.at[slot, g],
            device_id={"seq": right},
            device_id_type=MESH,
        )

    q_copy = pltpu.make_async_copy(q_hbm.at[0], q, q_sem)

    barrier = pltpu.get_barrier_semaphore()

    @pl.when(me > 0)
    def _():
        pl.semaphore_signal(barrier, inc=1, device_id={"seq": left}, device_id_type=MESH)

    for g in range(groups):
        for copy in loads(g):
            copy.start()
    q_copy.start()

    @pl.when(me < n - 1)
    def _():
        pl.semaphore_wait(barrier, 1)

    for g in range(groups):
        for copy in loads(g):
            copy.wait()

        @pl.when(me < n - 1)
        def _():
            send(0, g).start()

    q_copy.wait()

    def scores_of(slot, g):
        stacked = jnp.concatenate(
            [
                q[:, (g * per_group + h) * HEAD_SIZE : (g * per_group + h + 1) * HEAD_SIZE]
                for h in range(per_group)
            ],
            axis=0,
        )
        return lax.dot_general(
            stacked,
            kv[slot, g, :rows, :],
            (((1,), (1,)), ((), ())),
            preferred_element_type=jnp.float32,
        )

    def weighted(p, slot, g):
        block = jnp.concatenate(
            [kv[slot, g, rows:, :], jnp.ones((rows, HEAD_SIZE), jnp.bfloat16)], axis=1
        )
        return jnp.dot(p.astype(jnp.bfloat16), block, preferred_element_type=jnp.float32)

    def finish(total, g):
        done = (total[:, :HEAD_SIZE] / total[:, HEAD_SIZE:]).astype(jnp.bfloat16)
        for h in range(per_group):
            at = (g * per_group + h) * HEAD_SIZE
            o[0, :, at : at + HEAD_SIZE] = done[h * rows : (h + 1) * rows]

    row = lax.rem(lax.broadcasted_iota(jnp.int32, (per_group * rows, rows), 0), rows)
    visible = lax.broadcasted_iota(jnp.int32, (per_group * rows, rows), 1) <= row

    for g in range(groups):
        s = jnp.where(visible, scores_of(0, g), -1e30)
        new_m = jnp.max(s, axis=1, keepdims=True)
        total = weighted(jnp.exp2((s - new_m) * SCALE), 0, g)
        acc[g] = total
        m[g] = jnp.broadcast_to(new_m, m.shape[1:])

        @pl.when(me == 0)
        def _():
            finish(acc[g], g)

    @pl.loop(1, me + 1)
    def _(slot):
        for g in range(groups):
            receive(slot, g).wait_recv()

            @pl.when(me < n - 1)
            def _():
                send(slot, g).start()

            s = scores_of(slot, g)
            old_m = m[g]
            new_m = jnp.maximum(old_m, jnp.max(s, axis=1, keepdims=True))
            fade = jnp.exp2((old_m - new_m) * SCALE)
            p = jnp.exp2((s - new_m[:, :1]) * SCALE)
            total = acc[g] * jnp.concatenate([fade, fade], axis=1) + weighted(p, slot, g)

            @pl.when(slot < me)
            def _():
                acc[g] = total
                m[g] = new_m

            @pl.when(slot == me)
            def _():
                finish(total, g)

    @pl.when(me < n - 1)
    def _():
        @pl.loop(0, me + 1)
        def _(slot):
            for g in range(groups):
                send(slot, g).wait_send()


def on_device(n, queries, keys, values):
    rows, query_width = queries.shape[1:]
    groups = keys.shape[2] // HEAD_SIZE
    per_group = query_width // HEAD_SIZE // groups
    hbm = pl.BlockSpec(memory_space=pltpu.HBM)
    held = (2 * rows * query_width + 2 * n * rows * keys.shape[2]) * 2 + 3 * rows * query_width * 4
    return pl.pallas_call(
        functools.partial(kernel, n, groups, per_group),
        out_shape=jax.ShapeDtypeStruct(queries.shape, queries.dtype),
        in_specs=[hbm, hbm, hbm],
        out_specs=pl.BlockSpec(memory_space=pltpu.VMEM),
        scratch_shapes=[
            pltpu.VMEM((rows, query_width), jnp.bfloat16),
            pltpu.VMEM((n, groups, 2 * rows, HEAD_SIZE), jnp.bfloat16),
            pltpu.VMEM((groups, per_group * rows, HEAD_SIZE), jnp.float32),
            pltpu.VMEM((groups, per_group * rows, 2 * HEAD_SIZE), jnp.float32),
            pltpu.SemaphoreType.DMA((2, groups)),
            pltpu.SemaphoreType.DMA,
            pltpu.SemaphoreType.DMA((n, groups)),
            pltpu.SemaphoreType.DMA((n, groups)),
        ],
        compiler_params=pltpu.CompilerParams(collective_id=0, has_side_effects=True, vmem_limit_bytes=held + 4 * 2**20),
    )(*(pltpu.with_memory_space_constraint(x, pltpu.HBM) for x in (queries, keys, values)))


def solution(mesh):
    spec = P(("groups", "batch"), "seq", None)
    n = mesh.shape["seq"]
    return jax.shard_map(
        functools.partial(scheduled if n <= SCHEDULED else on_device, n),
        mesh=mesh,
        in_specs=(spec, spec, spec),
        out_specs=spec,
        check_vma=False,
    )
```

```python
import functools
import math

import jax
import jax.numpy as jnp
from jax import lax
from jax.experimental import pallas as pl
from jax.experimental.pallas import tpu as pltpu
from jax.sharding import PartitionSpec as P

HEAD_SIZE = 128
SCALE = math.log2(math.e) / math.sqrt(HEAD_SIZE)
MESH = pl.DeviceIdType.MESH

SCHEDULED = 4

FIRST, NEXT, MERGE = range(3)
KEEP, FINISH, RETURN = range(3)
CODE = 2**14


def pack(op, slot, g, answer=0, wait=0, forward=0, then=0, flag=KEEP):
    code = 0
    for value, size in ((flag, 4), (then, 8), (forward, 2), (wait, 2), (answer, 2), (g, 4), (slot, 4), (op, 4)):
        code = code * size + value
    return code


def moved_heads(n, groups, phase):
    return 0 if n < 4 else groups // (2 if phase == 0 else 4)


def order_of(top, groups, moved, phase):
    stay = list(range(moved, groups))
    older = range(top - 1, -1, -1)
    if phase == 0 and moved:
        out = [(top, 0)] + [(top, g) for g in stay] + [(b, 0) for b in older]
        for g in range(1, moved):
            out += [(b, g) for b in range(top, -1, -1)]
        return out + [(b, g) for b in older for g in stay]
    ahead = [(top, g) for g in stay[1:]]
    out = [(top, stay[0])]
    behind = [(b, g) for b in older for g in stay[1:] + stay[:1]]
    for i, unit in enumerate(behind):
        out += [unit] + (ahead[i - 1 : i] if 0 < i else [])
    out += ahead[max(len(behind) - 1, 0) :]
    for g in range(moved):
        out += [(b, g) for b in [*older, top]]
    return out


def script(n, groups, phase, rank):
    moved = moved_heads(n, groups, phase)
    helper, last = n - 2, n - 1
    order = order_of(max(n - 3, 0), groups, moved, phase)

    def sends(r):
        mine = [(b, g) for b, g in order if b <= r]
        if r < helper:
            return mine
        own = [(r, g) for g in range(moved, groups)]
        return own + [(b, g) for b, g in mine if g >= moved]

    queue = sends(rank) if rank < last else []
    arrivals = sends(helper) if rank == last else [(b, g) for b, g in order if b < rank]
    before = []
    while queue and queue[0][0] == rank:
        before.append(queue.pop(0)[1])

    steps = []
    left = {g: rank for g in range(groups)}
    waiting = {g: rank for g in range(moved)} if rank == helper else {}
    seen = {g: [] for g in waiting}
    ready = set()
    returned = 0

    def start_answer(g):
        ready.add(g)
        steps.append(pack(FIRST, 0, g, answer=1))
        for slot in seen[g]:
            steps.append(pack(NEXT, slot, g, answer=1))

    for i, (b, g) in enumerate(arrivals):
        slot = rank - b
        how = dict(wait=1)
        if queue and queue[0] == (b, g):
            queue.pop(0)
            how["forward"] = 1
            if queue and queue[0][0] == rank:
                how["then"] = queue.pop(0)[1] + 1
        left[g] -= 1
        if g in waiting:
            waiting[g] -= 1
            if g in ready:
                steps.append(pack(NEXT, slot, g, answer=1, flag=KEEP if waiting[g] else RETURN, **how))
                how = {}
            seen[g].append(slot)
        ends = left[g] == 0 and not (rank == last and g < moved)
        steps.append(pack(NEXT, slot, g, flag=FINISH if ends else KEEP, **how))
        if i + 1 < len(arrivals):
            h = arrivals[i + 1][1]
            if h in waiting and waiting[h] == 1:
                start_answer(h)
        if rank == last:
            while returned < moved and returns_before(order, moved, returned, groups) <= i + 1:
                steps.append(pack(MERGE, 0, returned))
                returned += 1
    if rank == last:
        steps += [pack(MERGE, 0, g) for g in range(returned, moved)]
    assert not queue
    return before, steps


def returns_before(order, moved, g, groups):
    at = max(i for i, (_, h) in enumerate(order) if h == g)
    return groups - moved + sum(1 for _, h in order[:at] if h >= moved)


def scheduled_kernel(
    n, groups, per_group, most,
    q_hbm, k_hbm, v_hbm, o,
    q, qt, kv, m, l, acc, back, back_stats, mine, mine_stats,
    load_sem, q_sem, send_sem, recv_sem, ask_send, ask_recv, back_send, back_recv,
):
    rows = kv.shape[2] // 2
    tall = per_group * HEAD_SIZE
    wide = per_group * rows
    me = lax.axis_index("seq")
    phase = lax.rem(lax.axis_index("batch"), 2)
    last, helper = n - 1, n - 2

    def kv_load(g):
        cols = pl.ds(g * HEAD_SIZE, HEAD_SIZE)
        return (
            pltpu.make_async_copy(
                k_hbm.at[0, :, cols], kv.at[0, g, pl.ds(0, rows)], load_sem.at[0, g]
            ),
            pltpu.make_async_copy(
                v_hbm.at[0, :, cols], kv.at[0, g, pl.ds(rows, rows)], load_sem.at[1, g]
            ),
        )

    def q_load(g):
        cols = pl.ds(g * tall, tall)
        return pltpu.make_async_copy(q_hbm.at[0, :, cols], q.at[g], q_sem.at[g])

    def send(slot, g):
        return pltpu.make_async_remote_copy(
            src_ref=kv.at[slot, g],
            dst_ref=kv.at[slot + 1, g],
            send_sem=send_sem.at[slot, g],
            recv_sem=recv_sem.at[slot + 1, g],
            device_id={"seq": jnp.minimum(me + 1, last)},
            device_id_type=MESH,
        )

    def receive(slot, g):
        return pltpu.make_async_remote_copy(
            src_ref=kv.at[slot, g],
            dst_ref=kv.at[slot, g],
            send_sem=send_sem.at[slot, g],
            recv_sem=recv_sem.at[slot, g],
            device_id={"seq": jnp.minimum(me + 1, last)},
            device_id_type=MESH,
        )

    def ask(g):
        return pltpu.make_async_remote_copy(
            src_ref=q.at[g],
            dst_ref=q.at[groups + g],
            send_sem=ask_send.at[g],
            recv_sem=ask_recv.at[g],
            device_id={"seq": jnp.int32(helper)},
            device_id_type=MESH,
        )

    def give(g):
        return (
            pltpu.make_async_remote_copy(
                src_ref=mine.at[g],
                dst_ref=back.at[g],
                send_sem=back_send.at[0, g],
                recv_sem=back_recv.at[0, g],
                device_id={"seq": jnp.int32(last)},
                device_id_type=MESH,
            ),
            pltpu.make_async_remote_copy(
                src_ref=mine_stats.at[g],
                dst_ref=back_stats.at[g],
                send_sem=back_send.at[1, g],
                recv_sem=back_recv.at[1, g],
                device_id={"seq": jnp.int32(last)},
                device_id_type=MESH,
            ),
        )

    barrier = pltpu.get_barrier_semaphore()

    @pl.when(me > 0)
    def _():
        pl.semaphore_signal(barrier, inc=1, device_id={"seq": me - 1}, device_id_type=MESH)

    if most:
        @pl.when(me == helper)
        def _():
            pl.semaphore_signal(barrier, inc=1, device_id={"seq": jnp.int32(last)}, device_id_type=MESH)

    for g in range(groups):
        for copy in kv_load(g):
            copy.start()
    for g in range(groups):
        q_load(g).start()

    scripts = {(r, p): script(n, groups, p, r) for r in range(n) for p in range(2)}
    here = {key: (me == key[0]) & (phase == key[1]) for key in scripts}

    def pick(values):
        out = jnp.int32(0)
        for key, value in values.items():
            if value:
                out = jnp.where(here[key], jnp.int32(value), out)
        return out

    count = pick({key: len(steps) for key, (_, steps) in scripts.items()})
    longest = max(len(steps) for _, steps in scripts.values())
    words = []
    for at in range(0, longest, 2):
        pairs = {key: (steps[at : at + 2] + [0, 0])[:2] for key, (_, steps) in scripts.items()}
        words.append(pick({key: low + CODE * high for key, (low, high) in pairs.items()}))

    @pl.when(me < last if not most else me >= 0)
    def _():
        pl.semaphore_wait(barrier, 1)

    for key, (before, _) in scripts.items():
        rank, p = key

        @pl.when(here[key])
        def _(rank=rank, p=p, before=before):
            if rank == last:
                for g in range(moved_heads(n, groups, p)):
                    q_load(g).wait()
                    ask(g).start()
            for g in before:
                for copy in kv_load(g):
                    copy.wait()
                send(0, g).start()
            for g in range(groups):
                if g not in before:
                    for copy in kv_load(g):
                        copy.wait()
            for g in range(groups):
                if rank < last or g >= moved_heads(n, groups, p):
                    q_load(g).wait()

    def scores_of(slot, g, turned):
        return jnp.dot(kv[slot, g, :rows, :], turned, preferred_element_type=jnp.float32)

    def weighted(p, slot, g):
        return jnp.dot(
            kv[slot, g, rows:, :].T, p.astype(jnp.bfloat16), preferred_element_type=jnp.float32
        )

    def write(total, g):
        done = total.astype(jnp.bfloat16)
        for h in range(per_group):
            at = pl.multiple_of((g * per_group + h) * HEAD_SIZE, HEAD_SIZE)
            o[0, :, pl.ds(at, HEAD_SIZE)] = done[:, h * rows : (h + 1) * rows].T

    def conclude(qi, g, flag):
        @pl.when(flag == FINISH)
        def _():
            write(acc[qi] / l[qi], g)

        if most:
            @pl.when(flag == RETURN)
            def _():
                mine[g] = (acc[qi] / l[qi]).astype(jnp.bfloat16)
                mine_stats[g, 0:1] = m[qi]
                mine_stats[g, 1:2] = l[qi]
                for copy in give(g):
                    copy.start()

    key = lax.broadcasted_iota(jnp.int32, (rows, wide), 0)
    query = lax.rem(lax.broadcasted_iota(jnp.int32, (rows, wide), 1), rows)

    @pl.loop(0, groups + count)
    def _(i):
        at = jnp.maximum(i - groups, 0)
        word = words[0] if words else jnp.int32(0)
        for j, other in enumerate(words[1:]):
            word = jnp.where(at >= 2 * (j + 1), other, word)
        code = jnp.where(lax.rem(at, 2) == 0, lax.rem(word, CODE), lax.div(word, CODE))
        own = pack(FIRST, 0, 0) + jnp.where(me == 0, pack(FIRST, 0, 0, flag=FINISH), 0) + pack(FIRST, 0, 1) * i
        code = jnp.where(i < groups, own, code)
        op = lax.rem(code, 4)
        slot = lax.rem(lax.div(code, 4), 4)
        g = lax.rem(lax.div(code, 16), 4)
        answer = lax.rem(lax.div(code, 64), 2)
        wait = lax.rem(lax.div(code, 128), 2)
        forward = lax.rem(lax.div(code, 256), 2)
        then = lax.rem(lax.div(code, 512), 8)
        flag = lax.div(code, 4096)
        qi = g + groups * answer

        @pl.when(wait == 1)
        def _():
            receive(slot, g).wait_recv()

            @pl.when(forward == 1)
            def _():
                send(slot, g).start()

            @pl.when(then > 0)
            def _():
                send(0, then - 1).start()

        if most:
            @pl.when((op == FIRST) & (answer == 1))
            def _():
                ask(g).wait_recv()

        @pl.when(op == FIRST)
        def _():
            for h in range(per_group):
                qt[qi, :, h * rows : (h + 1) * rows] = q[qi, :, h * HEAD_SIZE : (h + 1) * HEAD_SIZE].T
            s = jnp.where(key <= query + rows * answer, scores_of(0, g, qt[qi]), -1e30)
            new_m = jnp.max(s, axis=0, keepdims=True)
            p = jnp.exp2((s - new_m) * SCALE)
            m[qi] = new_m
            l[qi] = jnp.sum(p, axis=0, keepdims=True)
            acc[qi] = weighted(p, 0, g)
            conclude(qi, g, flag)

        @pl.when(op == NEXT)
        def _():
            s = scores_of(slot, g, qt[qi])
            old_m = m[qi]
            new_m = jnp.maximum(old_m, jnp.max(s, axis=0, keepdims=True))
            fade = jnp.exp2((old_m - new_m) * SCALE)
            p = jnp.exp2((s - new_m) * SCALE)
            m[qi] = new_m
            l[qi] = l[qi] * fade + jnp.sum(p, axis=0, keepdims=True)
            acc[qi] = acc[qi] * fade + weighted(p, slot, g)
            conclude(qi, g, flag)

        if most:
            @pl.when(op == MERGE)
            def _():
                for copy in give(g):
                    copy.wait_recv()
                here, there = m[g], back_stats[g, 0:1]
                new_m = jnp.maximum(here, there)
                fade = jnp.exp2((here - new_m) * SCALE)
                weight = jnp.exp2((there - new_m) * SCALE) * back_stats[g, 1:2]
                total = acc[g] * fade + back[g].astype(jnp.float32) * weight
                write(total / (l[g] * fade + weight), g)

    for p in range(2):
        away = moved_heads(n, groups, p)

        @pl.when((me < last) & (phase == p))
        def _(away=away):
            @pl.loop(0, me + 1)
            def _(slot):
                for g in range(groups):
                    if g < away:
                        @pl.when(me < helper)
                        def _():
                            send(slot, g).wait_send()
                    else:
                        send(slot, g).wait_send()

        for g in range(away):
            @pl.when((me == last) & (phase == p))
            def _(g=g):
                ask(g).wait_send()

            @pl.when((me == helper) & (phase == p))
            def _(g=g):
                for copy in give(g):
                    copy.wait_send()


def scheduled(n, queries, keys, values):
    rows, query_width = queries.shape[1:]
    groups = keys.shape[2] // HEAD_SIZE
    per_group = query_width // HEAD_SIZE // groups
    tall, wide = per_group * HEAD_SIZE, per_group * rows
    most = max(moved_heads(n, groups, p) for p in range(2))
    held = max(most, 1)
    hbm = pl.BlockSpec(memory_space=pltpu.HBM)
    total = groups + most
    bytes_held = (
        2 * rows * query_width * 2
        + total * rows * tall * (2 + 2 + 4)
        + 2 * n * rows * keys.shape[2] * 2
        + 2 * held * rows * tall * 2
        + (2 * total + 4 * held) * 8 * wide * 4
    )
    return pl.pallas_call(
        functools.partial(scheduled_kernel, n, groups, per_group, most),
        out_shape=jax.ShapeDtypeStruct(queries.shape, queries.dtype),
        in_specs=[hbm, hbm, hbm],
        out_specs=pl.BlockSpec(memory_space=pltpu.VMEM),
        scratch_shapes=[
            pltpu.VMEM((total, rows, tall), jnp.bfloat16),
            pltpu.VMEM((total, HEAD_SIZE, wide), jnp.bfloat16),
            pltpu.VMEM((n, groups, 2 * rows, HEAD_SIZE), jnp.bfloat16),
            pltpu.VMEM((total, 1, wide), jnp.float32),
            pltpu.VMEM((total, 1, wide), jnp.float32),
            pltpu.VMEM((total, HEAD_SIZE, wide), jnp.float32),
            pltpu.VMEM((held, HEAD_SIZE, wide), jnp.bfloat16),
            pltpu.VMEM((held, 2, wide), jnp.float32),
            pltpu.VMEM((held, HEAD_SIZE, wide), jnp.bfloat16),
            pltpu.VMEM((held, 2, wide), jnp.float32),
            pltpu.SemaphoreType.DMA((2, groups)),
            pltpu.SemaphoreType.DMA((groups,)),
            pltpu.SemaphoreType.DMA((n, groups)),
            pltpu.SemaphoreType.DMA((n, groups)),
            pltpu.SemaphoreType.DMA((held,)),
            pltpu.SemaphoreType.DMA((held,)),
            pltpu.SemaphoreType.DMA((2, held)),
            pltpu.SemaphoreType.DMA((2, held)),
        ],
        compiler_params=pltpu.CompilerParams(
            collective_id=0, has_side_effects=True, vmem_limit_bytes=bytes_held + 4 * 2**20
        ),
    )(*(pltpu.with_memory_space_constraint(x, pltpu.HBM) for x in (queries, keys, values)))


def kernel(
    n, groups, per_group,
    q_hbm, k_hbm, v_hbm, o,
    q, kv, m, acc,
    load_sem, q_sem, send_sem, recv_sem,
):
    rows = q.shape[0]
    me = lax.axis_index("seq")
    right, left = lax.rem(me + 1, n), lax.rem(me + n - 1, n)

    def loads(g):
        cols = pl.ds(g * HEAD_SIZE, HEAD_SIZE)
        return (
            pltpu.make_async_copy(
                k_hbm.at[0, :, cols], kv.at[0, g, pl.ds(0, rows)], load_sem.at[0, g]
            ),
            pltpu.make_async_copy(
                v_hbm.at[0, :, cols], kv.at[0, g, pl.ds(rows, rows)], load_sem.at[1, g]
            ),
        )

    def send(slot, g):
        return pltpu.make_async_remote_copy(
            src_ref=kv.at[slot, g],
            dst_ref=kv.at[slot + 1, g],
            send_sem=send_sem.at[slot, g],
            recv_sem=recv_sem.at[slot + 1, g],
            device_id={"seq": right},
            device_id_type=MESH,
        )

    def receive(slot, g):
        return pltpu.make_async_remote_copy(
            src_ref=kv.at[slot, g],
            dst_ref=kv.at[slot, g],
            send_sem=send_sem.at[slot, g],
            recv_sem=recv_sem.at[slot, g],
            device_id={"seq": right},
            device_id_type=MESH,
        )

    q_copy = pltpu.make_async_copy(q_hbm.at[0], q, q_sem)

    barrier = pltpu.get_barrier_semaphore()

    @pl.when(me > 0)
    def _():
        pl.semaphore_signal(barrier, inc=1, device_id={"seq": left}, device_id_type=MESH)

    for g in range(groups):
        for copy in loads(g):
            copy.start()
    q_copy.start()

    @pl.when(me < n - 1)
    def _():
        pl.semaphore_wait(barrier, 1)

    for g in range(groups):
        for copy in loads(g):
            copy.wait()

        @pl.when(me < n - 1)
        def _():
            send(0, g).start()

    q_copy.wait()

    def scores_of(slot, g):
        stacked = jnp.concatenate(
            [
                q[:, (g * per_group + h) * HEAD_SIZE : (g * per_group + h + 1) * HEAD_SIZE]
                for h in range(per_group)
            ],
            axis=0,
        )
        return lax.dot_general(
            stacked,
            kv[slot, g, :rows, :],
            (((1,), (1,)), ((), ())),
            preferred_element_type=jnp.float32,
        )

    def weighted(p, slot, g):
        block = jnp.concatenate(
            [kv[slot, g, rows:, :], jnp.ones((rows, HEAD_SIZE), jnp.bfloat16)], axis=1
        )
        return jnp.dot(p.astype(jnp.bfloat16), block, preferred_element_type=jnp.float32)

    def finish(total, g):
        done = (total[:, :HEAD_SIZE] / total[:, HEAD_SIZE:]).astype(jnp.bfloat16)
        for h in range(per_group):
            at = (g * per_group + h) * HEAD_SIZE
            o[0, :, at : at + HEAD_SIZE] = done[h * rows : (h + 1) * rows]

    row = lax.rem(lax.broadcasted_iota(jnp.int32, (per_group * rows, rows), 0), rows)
    visible = lax.broadcasted_iota(jnp.int32, (per_group * rows, rows), 1) <= row

    for g in range(groups):
        s = jnp.where(visible, scores_of(0, g), -1e30)
        new_m = jnp.max(s, axis=1, keepdims=True)
        total = weighted(jnp.exp2((s - new_m) * SCALE), 0, g)
        acc[g] = total
        m[g] = jnp.broadcast_to(new_m, m.shape[1:])

        @pl.when(me == 0)
        def _():
            finish(acc[g], g)

    @pl.loop(1, me + 1)
    def _(slot):
        for g in range(groups):
            receive(slot, g).wait_recv()

            @pl.when(me < n - 1)
            def _():
                send(slot, g).start()

            s = scores_of(slot, g)
            old_m = m[g]
            new_m = jnp.maximum(old_m, jnp.max(s, axis=1, keepdims=True))
            fade = jnp.exp2((old_m - new_m) * SCALE)
            p = jnp.exp2((s - new_m[:, :1]) * SCALE)
            total = acc[g] * jnp.concatenate([fade, fade], axis=1) + weighted(p, slot, g)

            @pl.when(slot < me)
            def _():
                acc[g] = total
                m[g] = new_m

            @pl.when(slot == me)
            def _():
                finish(total, g)

    @pl.when(me < n - 1)
    def _():
        @pl.loop(0, me + 1)
        def _(slot):
            for g in range(groups):
                send(slot, g).wait_send()


def on_device(n, queries, keys, values):
    rows, query_width = queries.shape[1:]
    groups = keys.shape[2] // HEAD_SIZE
    per_group = query_width // HEAD_SIZE // groups
    hbm = pl.BlockSpec(memory_space=pltpu.HBM)
    held = (2 * rows * query_width + 2 * n * rows * keys.shape[2]) * 2 + 3 * rows * query_width * 4
    return pl.pallas_call(
        functools.partial(kernel, n, groups, per_group),
        out_shape=jax.ShapeDtypeStruct(queries.shape, queries.dtype),
        in_specs=[hbm, hbm, hbm],
        out_specs=pl.BlockSpec(memory_space=pltpu.VMEM),
        scratch_shapes=[
            pltpu.VMEM((rows, query_width), jnp.bfloat16),
            pltpu.VMEM((n, groups, 2 * rows, HEAD_SIZE), jnp.bfloat16),
            pltpu.VMEM((groups, per_group * rows, HEAD_SIZE), jnp.float32),
            pltpu.VMEM((groups, per_group * rows, 2 * HEAD_SIZE), jnp.float32),
            pltpu.SemaphoreType.DMA((2, groups)),
            pltpu.SemaphoreType.DMA,
            pltpu.SemaphoreType.DMA((n, groups)),
            pltpu.SemaphoreType.DMA((n, groups)),
        ],
        compiler_params=pltpu.CompilerParams(collective_id=0, has_side_effects=True, vmem_limit_bytes=held + 4 * 2**20),
    )(*(pltpu.with_memory_space_constraint(x, pltpu.HBM) for x in (queries, keys, values)))


def solution(mesh):
    spec = P(("groups", "batch"), "seq", None)
    n = mesh.shape["seq"]
    return jax.shard_map(
        functools.partial(scheduled if n <= SCHEDULED else on_device, n),
        mesh=mesh,
        in_specs=(spec, spec, spec),
        out_specs=spec,
        check_vma=False,
    )
```

```python
import functools
import math

import jax
import jax.numpy as jnp
from jax import lax
from jax.experimental import pallas as pl
from jax.experimental.pallas import tpu as pltpu
from jax.sharding import PartitionSpec as P

HEAD_SIZE = 128
SCALE = math.log2(math.e) / math.sqrt(HEAD_SIZE)
MESH = pl.DeviceIdType.MESH

SCHEDULED = 4

FIRST, NEXT, MERGE, REST = range(4)
KEEP, FINISH, RETURN = range(3)
CODE = 2**14


def pack(op, slot, g, answer=0, wait=0, forward=0, then=0, flag=KEEP):
    code = 0
    for value, size in ((flag, 4), (then, 8), (forward, 2), (wait, 2), (answer, 2), (g, 4), (slot, 4), (op, 4)):
        code = code * size + value
    return code


def moved_heads(n, groups, phase):
    return 0 if n < 4 else groups // (2 if phase == 0 else 4)


def order_of(top, groups, moved, phase):
    stay = list(range(moved, groups))
    older = range(top - 1, -1, -1)
    if phase == 0 and moved:
        out = [(top, 0)] + [(top, g) for g in stay] + [(b, 0) for b in older]
        for g in range(1, moved):
            out += [(b, g) for b in range(top, -1, -1)]
        return out + [(b, g) for b in older for g in stay]
    ahead = [(top, g) for g in stay[1:]]
    out = [(top, stay[0])]
    behind = [(b, g) for b in older for g in stay[1:] + stay[:1]]
    for i, unit in enumerate(behind):
        out += [unit] + (ahead[i - 1 : i] if 0 < i else [])
    out += ahead[max(len(behind) - 1, 0) :]
    for g in range(moved):
        out += [(b, g) for b in [*older, top]]
    return out


def script(n, groups, phase, rank):
    moved = moved_heads(n, groups, phase)
    helper, last = n - 2, n - 1
    order = order_of(max(n - 3, 0), groups, moved, phase)

    def sends(r):
        mine = [(b, g) for b, g in order if b <= r]
        if r < helper:
            return mine
        own = [(r, g) for g in range(moved, groups)]
        return own + [(b, g) for b, g in mine if g >= moved]

    queue = sends(rank) if rank < last else []
    arrivals = sends(helper) if rank == last else [(b, g) for b, g in order if b < rank]
    before = []
    while queue and queue[0][0] == rank:
        before.append(queue.pop(0)[1])

    steps = []
    left = {g: rank for g in range(groups)}
    waiting = {g: rank for g in range(moved)} if rank == helper else {}
    seen = {g: [] for g in waiting}
    ready = set()
    returned = 0

    def start_answer(g):
        ready.add(g)
        steps.append(pack(FIRST, 0, g, answer=1))
        for slot in seen[g]:
            steps.append(pack(NEXT, slot, g, answer=1))

    for i, (b, g) in enumerate(arrivals):
        slot = rank - b
        how = dict(wait=1)
        if queue and queue[0] == (b, g):
            queue.pop(0)
            how["forward"] = 1
            while queue and queue[0][0] == rank:
                if "then" in how:
                    steps.append(pack(REST, slot, g, **how))
                    how = {}
                how["then"] = queue.pop(0)[1] + 1
        left[g] -= 1
        if g in waiting:
            waiting[g] -= 1
            if g in ready:
                steps.append(pack(NEXT, slot, g, answer=1, flag=KEEP if waiting[g] else RETURN, **how))
                how = {}
            seen[g].append(slot)
        ends = left[g] == 0 and not (rank == last and g < moved)
        steps.append(pack(NEXT, slot, g, flag=FINISH if ends else KEEP, **how))
        if i + 1 < len(arrivals):
            h = arrivals[i + 1][1]
            if h in waiting and waiting[h] == 1:
                start_answer(h)
        if rank == last:
            while returned < moved and returns_before(order, moved, returned, groups) <= i + 1:
                steps.append(pack(MERGE, 0, returned))
                returned += 1
    if rank == last:
        steps += [pack(MERGE, 0, g) for g in range(returned, moved)]
    assert not queue
    return before, steps, len(arrivals)


def returns_before(order, moved, g, groups):
    at = max(i for i, (_, h) in enumerate(order) if h == g)
    return groups - moved + sum(1 for _, h in order[:at] if h >= moved)


def scheduled_kernel(
    n, groups, per_group, most,
    q_hbm, k_hbm, v_hbm, o,
    q, qt, kv, m, l, acc, back, back_stats, mine, mine_stats,
    load_sem, send_sem, aside_sem, recv_sem, stats_sem,
):
    rows = kv.shape[2] // 2
    tall = per_group * HEAD_SIZE
    wide = per_group * rows
    me = lax.axis_index("seq")
    phase = lax.rem(lax.axis_index("batch"), 2)
    last, helper = n - 1, n - 2

    def kv_load(g):
        cols = pl.ds(g * HEAD_SIZE, HEAD_SIZE)
        return (
            pltpu.make_async_copy(
                k_hbm.at[0, :, cols], kv.at[0, g, pl.ds(0, rows)], load_sem.at[0]
            ),
            pltpu.make_async_copy(
                v_hbm.at[0, :, cols], kv.at[0, g, pl.ds(rows, rows)], load_sem.at[0]
            ),
        )

    def q_load(g):
        cols = pl.ds(g * tall, tall)
        return pltpu.make_async_copy(q_hbm.at[0, :, cols], q.at[g], load_sem.at[1])

    scripts = {(r, p): script(n, groups, p, r) for r in range(n) for p in range(2)}
    here = {key: (me == key[0]) & (phase == key[1]) for key in scripts}

    def wait_for(ref, sem):
        pltpu.make_async_copy(ref, ref, sem).wait()

    def send(slot, g, nth):
        return pltpu.make_async_remote_copy(
            src_ref=kv.at[slot, g],
            dst_ref=kv.at[slot + 1, g],
            send_sem=send_sem.at[0],
            recv_sem=recv_sem.at[nth],
            device_id={"seq": jnp.minimum(me + 1, last)},
            device_id_type=MESH,
        )

    def arrived(ref, nth):
        pltpu.make_async_copy(ref, ref, recv_sem.at[nth]).wait()

    asked_at = scripts[helper, 0][2]
    given_at = jnp.where(phase == 0, scripts[last, 0][2], scripts[last, 1][2])

    def ask(g):
        return pltpu.make_async_remote_copy(
            src_ref=q.at[g],
            dst_ref=q.at[groups + g],
            send_sem=aside_sem.at[0],
            recv_sem=recv_sem.at[asked_at + g],
            device_id={"seq": jnp.int32(helper)},
            device_id_type=MESH,
        )

    def give(g):
        return (
            pltpu.make_async_remote_copy(
                src_ref=mine.at[g],
                dst_ref=back.at[g],
                send_sem=aside_sem.at[0],
                recv_sem=recv_sem.at[given_at + g],
                device_id={"seq": jnp.int32(last)},
                device_id_type=MESH,
            ),
            pltpu.make_async_remote_copy(
                src_ref=mine_stats.at[g],
                dst_ref=back_stats.at[g],
                send_sem=aside_sem.at[1],
                recv_sem=stats_sem.at[g],
                device_id={"seq": jnp.int32(last)},
                device_id_type=MESH,
            ),
        )

    barrier = pltpu.get_barrier_semaphore()

    @pl.when(me > 0)
    def _():
        pl.semaphore_signal(barrier, inc=1, device_id={"seq": me - 1}, device_id_type=MESH)

    if most:
        @pl.when(me == helper)
        def _():
            pl.semaphore_signal(barrier, inc=1, device_id={"seq": jnp.int32(last)}, device_id_type=MESH)

    for g in range(groups):
        for copy in kv_load(g):
            copy.start()
    for g in range(groups):
        q_load(g).start()

    def pick(values):
        out = jnp.int32(0)
        for key, value in values.items():
            if value:
                out = jnp.where(here[key], jnp.int32(value), out)
        return out

    count = pick({key: len(steps) for key, (_, steps, _) in scripts.items()})
    longest = max(len(steps) for _, steps, _ in scripts.values())
    words = []
    for at in range(0, longest, 2):
        pairs = {key: (steps[at : at + 2] + [0, 0])[:2] for key, (_, steps, _) in scripts.items()}
        words.append(pick({key: low + CODE * high for key, (low, high) in pairs.items()}))

    @pl.when(me < last if not most else me >= 0)
    def _():
        pl.semaphore_wait(barrier, 1)

    wait_for(kv.at[0], load_sem.at[0])

    for (rank, p), (before, _, _) in scripts.items():
        @pl.when(here[rank, p])
        def _(before=before):
            for i, g in enumerate(before):
                send(0, g, i).start()

    wait_for(q.at[pl.ds(0, groups)], load_sem.at[1])

    for p in range(2):
        for g in range(moved_heads(n, groups, p)):
            @pl.when(here[last, p])
            def _(g=g):
                ask(g).start()

    sent_before = pick({key: len(before) for key, (before, _, _) in scripts.items()})

    def scores_of(slot, g, turned):
        return jnp.dot(kv[slot, g, :rows, :], turned, preferred_element_type=jnp.float32)

    def weighted(p, slot, g):
        return jnp.dot(
            kv[slot, g, rows:, :].T, p.astype(jnp.bfloat16), preferred_element_type=jnp.float32
        )

    def write(total, g):
        done = total.astype(jnp.bfloat16)
        for h in range(per_group):
            at = pl.multiple_of((g * per_group + h) * HEAD_SIZE, HEAD_SIZE)
            o[0, :, pl.ds(at, HEAD_SIZE)] = done[:, h * rows : (h + 1) * rows].T

    def conclude(qi, g, flag):
        @pl.when(flag == FINISH)
        def _():
            write(acc[qi] * (1.0 / l[qi]), g)

        if most:
            @pl.when(flag == RETURN)
            def _():
                mine[g] = (acc[qi] * (1.0 / l[qi])).astype(jnp.bfloat16)
                mine_stats[g, 0:1] = m[qi]
                mine_stats[g, 1:2] = l[qi]
                for copy in give(g):
                    copy.start()

    key = lax.broadcasted_iota(jnp.int32, (rows, wide), 0)
    query = lax.rem(lax.broadcasted_iota(jnp.int32, (rows, wide), 1), rows)

    def step(i, counts):
        got, sent = counts
        at = jnp.maximum(i - groups, 0)
        word = words[0] if words else jnp.int32(0)
        for j, other in enumerate(words[1:]):
            word = jnp.where(at >= 2 * (j + 1), other, word)
        code = jnp.where(lax.rem(at, 2) == 0, lax.rem(word, CODE), lax.div(word, CODE))
        own = pack(FIRST, 0, 0) + jnp.where(me == 0, pack(FIRST, 0, 0, flag=FINISH), 0) + pack(FIRST, 0, 1) * i
        code = jnp.where(i < groups, own, code)
        op = lax.rem(code, 4)
        slot = lax.rem(lax.div(code, 4), 4)
        g = lax.rem(lax.div(code, 16), 4)
        answer = lax.rem(lax.div(code, 64), 2)
        wait = lax.rem(lax.div(code, 128), 2)
        forward = lax.rem(lax.div(code, 256), 2)
        then = lax.rem(lax.div(code, 512), 8)
        flag = lax.div(code, 4096)
        qi = g + groups * answer

        @pl.when(wait == 1)
        def _():
            arrived(kv.at[slot, g], got)

            @pl.when(forward == 1)
            def _():
                send(slot, g, sent).start()

        sent = sent + forward

        @pl.when(then > 0)
        def _():
            send(0, then - 1, sent).start()

        if most:
            @pl.when((op == FIRST) & (answer == 1))
            def _():
                arrived(q.at[groups + g], asked_at + g)

        @pl.when(op == FIRST)
        def _():
            for h in range(per_group):
                qt[qi, :, h * rows : (h + 1) * rows] = q[qi, :, h * HEAD_SIZE : (h + 1) * HEAD_SIZE].T
            s = jnp.where(key <= query + rows * answer, scores_of(0, g, qt[qi]), -1e30)
            new_m = jnp.max(s, axis=0, keepdims=True)
            p = jnp.exp2((s - new_m) * SCALE)
            m[qi] = new_m
            l[qi] = jnp.sum(p, axis=0, keepdims=True)
            acc[qi] = weighted(p, 0, g)
            conclude(qi, g, flag)

        @pl.when(op == NEXT)
        def _():
            s = scores_of(slot, g, qt[qi])
            old_m = m[qi]
            new_m = jnp.maximum(old_m, jnp.max(s, axis=0, keepdims=True))
            fade = jnp.exp2((old_m - new_m) * SCALE)
            p = jnp.exp2((s - new_m) * SCALE)
            m[qi] = new_m
            l[qi] = l[qi] * fade + jnp.sum(p, axis=0, keepdims=True)
            acc[qi] = acc[qi] * fade + weighted(p, slot, g)
            conclude(qi, g, flag)

        if most:
            @pl.when(op == MERGE)
            def _():
                arrived(back.at[g], given_at + g)
                wait_for(back_stats.at[g], stats_sem.at[g])
                here, there = m[g], back_stats[g, 0:1]
                new_m = jnp.maximum(here, there)
                fade = jnp.exp2((here - new_m) * SCALE)
                weight = jnp.exp2((there - new_m) * SCALE) * back_stats[g, 1:2]
                share = 1.0 / (l[g] * fade + weight)
                write(acc[g] * (fade * share) + back[g].astype(jnp.float32) * (weight * share), g)

        return got + wait, sent + jnp.where(then > 0, 1, 0)

    lax.fori_loop(0, groups + count, step, (jnp.int32(0), sent_before))

    for (rank, p) in scripts:
        away = moved_heads(n, groups, p)

        @pl.when(here[rank, p])
        def _(rank=rank, away=away):
            if rank < helper:
                wait_for(kv.at[pl.ds(0, rank + 1)], send_sem.at[0])
            elif rank == helper:
                wait_for(kv.at[pl.ds(0, rank + 1), pl.ds(away, groups - away)], send_sem.at[0])
                if away:
                    wait_for(mine.at[pl.ds(0, away)], aside_sem.at[0])
                    wait_for(mine_stats.at[pl.ds(0, away)], aside_sem.at[1])
            elif away:
                wait_for(q.at[pl.ds(0, away)], aside_sem.at[0])


def scheduled(n, queries, keys, values):
    rows, query_width = queries.shape[1:]
    groups = keys.shape[2] // HEAD_SIZE
    per_group = query_width // HEAD_SIZE // groups
    tall, wide = per_group * HEAD_SIZE, per_group * rows
    most = max(moved_heads(n, groups, p) for p in range(2))
    held = max(most, 1)
    hbm = pl.BlockSpec(memory_space=pltpu.HBM)
    total = groups + most
    received = max(
        script(n, groups, p, r)[2] + (moved_heads(n, groups, p) if r >= n - 2 else 0)
        for p in range(2)
        for r in range(n)
    )
    bytes_held = (
        2 * rows * query_width * 2
        + total * rows * tall * (2 + 2 + 4)
        + 2 * n * rows * keys.shape[2] * 2
        + 2 * held * rows * tall * 2
        + (2 * total + 4 * held) * 8 * wide * 4
    )
    return pl.pallas_call(
        functools.partial(scheduled_kernel, n, groups, per_group, most),
        out_shape=jax.ShapeDtypeStruct(queries.shape, queries.dtype),
        in_specs=[hbm, hbm, hbm],
        out_specs=pl.BlockSpec(memory_space=pltpu.VMEM),
        scratch_shapes=[
            pltpu.VMEM((total, rows, tall), jnp.bfloat16),
            pltpu.VMEM((total, HEAD_SIZE, wide), jnp.bfloat16),
            pltpu.VMEM((n, groups, 2 * rows, HEAD_SIZE), jnp.bfloat16),
            pltpu.VMEM((total, 1, wide), jnp.float32),
            pltpu.VMEM((total, 1, wide), jnp.float32),
            pltpu.VMEM((total, HEAD_SIZE, wide), jnp.float32),
            pltpu.VMEM((held, HEAD_SIZE, wide), jnp.bfloat16),
            pltpu.VMEM((held, 2, wide), jnp.float32),
            pltpu.VMEM((held, HEAD_SIZE, wide), jnp.bfloat16),
            pltpu.VMEM((held, 2, wide), jnp.float32),
            pltpu.SemaphoreType.DMA((2,)),
            pltpu.SemaphoreType.DMA((1,)),
            pltpu.SemaphoreType.DMA((2,)),
            pltpu.SemaphoreType.DMA((received,)),
            pltpu.SemaphoreType.DMA((held,)),
        ],
        compiler_params=pltpu.CompilerParams(
            collective_id=0, has_side_effects=True, vmem_limit_bytes=bytes_held + 4 * 2**20
        ),
    )(*(pltpu.with_memory_space_constraint(x, pltpu.HBM) for x in (queries, keys, values)))


def kernel(
    n, groups, per_group,
    q_hbm, k_hbm, v_hbm, o,
    q, kv, m, acc,
    load_sem, q_sem, send_sem, recv_sem,
):
    rows = q.shape[0]
    me = lax.axis_index("seq")
    right, left = lax.rem(me + 1, n), lax.rem(me + n - 1, n)

    def loads(g):
        cols = pl.ds(g * HEAD_SIZE, HEAD_SIZE)
        return (
            pltpu.make_async_copy(
                k_hbm.at[0, :, cols], kv.at[0, g, pl.ds(0, rows)], load_sem.at[0, g]
            ),
            pltpu.make_async_copy(
                v_hbm.at[0, :, cols], kv.at[0, g, pl.ds(rows, rows)], load_sem.at[1, g]
            ),
        )

    def send(slot, g):
        return pltpu.make_async_remote_copy(
            src_ref=kv.at[slot, g],
            dst_ref=kv.at[slot + 1, g],
            send_sem=send_sem.at[slot, g],
            recv_sem=recv_sem.at[slot + 1, g],
            device_id={"seq": right},
            device_id_type=MESH,
        )

    def receive(slot, g):
        return pltpu.make_async_remote_copy(
            src_ref=kv.at[slot, g],
            dst_ref=kv.at[slot, g],
            send_sem=send_sem.at[slot, g],
            recv_sem=recv_sem.at[slot, g],
            device_id={"seq": right},
            device_id_type=MESH,
        )

    q_copy = pltpu.make_async_copy(q_hbm.at[0], q, q_sem)

    barrier = pltpu.get_barrier_semaphore()

    @pl.when(me > 0)
    def _():
        pl.semaphore_signal(barrier, inc=1, device_id={"seq": left}, device_id_type=MESH)

    for g in range(groups):
        for copy in loads(g):
            copy.start()
    q_copy.start()

    @pl.when(me < n - 1)
    def _():
        pl.semaphore_wait(barrier, 1)

    for g in range(groups):
        for copy in loads(g):
            copy.wait()

        @pl.when(me < n - 1)
        def _():
            send(0, g).start()

    q_copy.wait()

    def scores_of(slot, g):
        stacked = jnp.concatenate(
            [
                q[:, (g * per_group + h) * HEAD_SIZE : (g * per_group + h + 1) * HEAD_SIZE]
                for h in range(per_group)
            ],
            axis=0,
        )
        return lax.dot_general(
            stacked,
            kv[slot, g, :rows, :],
            (((1,), (1,)), ((), ())),
            preferred_element_type=jnp.float32,
        )

    def weighted(p, slot, g):
        block = jnp.concatenate(
            [kv[slot, g, rows:, :], jnp.ones((rows, HEAD_SIZE), jnp.bfloat16)], axis=1
        )
        return jnp.dot(p.astype(jnp.bfloat16), block, preferred_element_type=jnp.float32)

    def finish(total, g):
        done = (total[:, :HEAD_SIZE] / total[:, HEAD_SIZE:]).astype(jnp.bfloat16)
        for h in range(per_group):
            at = (g * per_group + h) * HEAD_SIZE
            o[0, :, at : at + HEAD_SIZE] = done[h * rows : (h + 1) * rows]

    row = lax.rem(lax.broadcasted_iota(jnp.int32, (per_group * rows, rows), 0), rows)
    visible = lax.broadcasted_iota(jnp.int32, (per_group * rows, rows), 1) <= row

    for g in range(groups):
        s = jnp.where(visible, scores_of(0, g), -1e30)
        new_m = jnp.max(s, axis=1, keepdims=True)
        total = weighted(jnp.exp2((s - new_m) * SCALE), 0, g)
        acc[g] = total
        m[g] = jnp.broadcast_to(new_m, m.shape[1:])

        @pl.when(me == 0)
        def _():
            finish(acc[g], g)

    @pl.loop(1, me + 1)
    def _(slot):
        for g in range(groups):
            receive(slot, g).wait_recv()

            @pl.when(me < n - 1)
            def _():
                send(slot, g).start()

            s = scores_of(slot, g)
            old_m = m[g]
            new_m = jnp.maximum(old_m, jnp.max(s, axis=1, keepdims=True))
            fade = jnp.exp2((old_m - new_m) * SCALE)
            p = jnp.exp2((s - new_m[:, :1]) * SCALE)
            total = acc[g] * jnp.concatenate([fade, fade], axis=1) + weighted(p, slot, g)

            @pl.when(slot < me)
            def _():
                acc[g] = total
                m[g] = new_m

            @pl.when(slot == me)
            def _():
                finish(total, g)

    @pl.when(me < n - 1)
    def _():
        @pl.loop(0, me + 1)
        def _(slot):
            for g in range(groups):
                send(slot, g).wait_send()


def on_device(n, queries, keys, values):
    rows, query_width = queries.shape[1:]
    groups = keys.shape[2] // HEAD_SIZE
    per_group = query_width // HEAD_SIZE // groups
    hbm = pl.BlockSpec(memory_space=pltpu.HBM)
    held = (2 * rows * query_width + 2 * n * rows * keys.shape[2]) * 2 + 3 * rows * query_width * 4
    return pl.pallas_call(
        functools.partial(kernel, n, groups, per_group),
        out_shape=jax.ShapeDtypeStruct(queries.shape, queries.dtype),
        in_specs=[hbm, hbm, hbm],
        out_specs=pl.BlockSpec(memory_space=pltpu.VMEM),
        scratch_shapes=[
            pltpu.VMEM((rows, query_width), jnp.bfloat16),
            pltpu.VMEM((n, groups, 2 * rows, HEAD_SIZE), jnp.bfloat16),
            pltpu.VMEM((groups, per_group * rows, HEAD_SIZE), jnp.float32),
            pltpu.VMEM((groups, per_group * rows, 2 * HEAD_SIZE), jnp.float32),
            pltpu.SemaphoreType.DMA((2, groups)),
            pltpu.SemaphoreType.DMA,
            pltpu.SemaphoreType.DMA((n, groups)),
            pltpu.SemaphoreType.DMA((n, groups)),
        ],
        compiler_params=pltpu.CompilerParams(collective_id=0, has_side_effects=True, vmem_limit_bytes=held + 4 * 2**20),
    )(*(pltpu.with_memory_space_constraint(x, pltpu.HBM) for x in (queries, keys, values)))


def solution(mesh):
    spec = P(("groups", "batch"), "seq", None)
    n = mesh.shape["seq"]
    return jax.shard_map(
        functools.partial(scheduled if n <= SCHEDULED else on_device, n),
        mesh=mesh,
        in_specs=(spec, spec, spec),
        out_specs=spec,
        check_vma=False,
    )
```

```python
import functools
import math

import jax
import jax.numpy as jnp
from jax import lax
from jax.experimental import pallas as pl
from jax.experimental.pallas import tpu as pltpu
from jax.sharding import PartitionSpec as P

HEAD_SIZE = 128
SCALE = math.log2(math.e) / math.sqrt(HEAD_SIZE)
MESH = pl.DeviceIdType.MESH

SCHEDULED = 4

FIRST, NEXT, MERGE, REST = range(4)
KEEP, FINISH, RETURN = range(3)
CODE = 2**14


def pack(op, slot, g, answer=0, wait=0, forward=0, then=0, flag=KEEP):
    code = 0
    for value, size in ((flag, 4), (then, 8), (forward, 2), (wait, 2), (answer, 2), (g, 4), (slot, 4), (op, 4)):
        code = code * size + value
    return code


def moved_heads(n, groups, phase):
    return 0 if n < 4 else groups // (2 if phase == 0 else 4)


def order_of(top, groups, moved, phase):
    stay = list(range(moved, groups))
    older = range(top - 1, -1, -1)
    if phase == 0 and moved:
        out = [(top, 0)] + [(top, g) for g in stay] + [(b, 0) for b in older]
        for g in range(1, moved):
            out += [(b, g) for b in range(top, -1, -1)]
        return out + [(b, g) for b in older for g in stay]
    ahead = [(top, g) for g in stay[1:]]
    out = [(top, stay[0])]
    behind = [(b, g) for b in older for g in stay[1:] + stay[:1]]
    for i, unit in enumerate(behind):
        out += [unit] + (ahead[i - 1 : i] if 0 < i else [])
    out += ahead[max(len(behind) - 1, 0) :]
    for g in range(moved):
        out += [(b, g) for b in [*older, top]]
    return out


def taken_up(phase, g):
    return 2 if phase else 2 + 2 * g


def script(n, groups, phase, rank):
    moved = moved_heads(n, groups, phase)
    helper, last = n - 2, n - 1
    order = order_of(max(n - 3, 0), groups, moved, phase)

    def sends(r):
        mine = [(b, g) for b, g in order if b <= r]
        if r < helper:
            return mine
        own = [(r, g) for g in range(moved, groups)]
        return own + [(b, g) for b, g in mine if g >= moved]

    queue = sends(rank) if rank < last else []
    arrivals = sends(helper) if rank == last else [(b, g) for b, g in order if b < rank]
    before = []
    while queue and queue[0][0] == rank:
        before.append(queue.pop(0)[1])

    steps = []
    left = {g: rank for g in range(groups)}
    waiting = {g: rank for g in range(moved)} if rank == helper else {}
    seen = {g: [] for g in waiting}
    ready = set()
    returned = 0

    def start_answer(g):
        ready.add(g)
        steps.append(pack(FIRST, 0, g, answer=1))
        for slot in seen[g]:
            steps.append(pack(NEXT, slot, g, answer=1))

    for i, (b, g) in enumerate(arrivals):
        slot = rank - b
        how = dict(wait=1)
        if queue and queue[0] == (b, g):
            queue.pop(0)
            how["forward"] = 1
            while queue and queue[0][0] == rank:
                if "then" in how:
                    steps.append(pack(REST, slot, g, **how))
                    how = {}
                how["then"] = queue.pop(0)[1] + 1
        left[g] -= 1
        if g in waiting:
            waiting[g] -= 1
            if g in ready:
                steps.append(pack(NEXT, slot, g, answer=1, flag=KEEP if waiting[g] else RETURN, **how))
                how = {}
            seen[g].append(slot)
        ends = left[g] == 0 and not (rank == last and g < moved)
        steps.append(pack(NEXT, slot, g, flag=FINISH if ends else KEEP, **how))
        for h in waiting:
            due = i + 1 < len(arrivals) and arrivals[i + 1][1] == h and waiting[h] == 1
            if h not in ready and (due or i >= taken_up(phase, h)):
                start_answer(h)
        if rank == last:
            while returned < moved and returns_before(order, moved, returned, groups) <= i + 1:
                steps.append(pack(MERGE, 0, returned))
                returned += 1
    if rank == last:
        steps += [pack(MERGE, 0, g) for g in range(returned, moved)]
    assert not queue
    return before, steps, len(arrivals)


def returns_before(order, moved, g, groups):
    at = max(i for i, (_, h) in enumerate(order) if h == g)
    return groups - moved + sum(1 for _, h in order[:at] if h >= moved)


def scheduled_kernel(
    n, groups, per_group, most,
    q_hbm, k_hbm, v_hbm, o,
    q, qt, kv, m, l, acc, back, back_stats, mine, mine_stats,
    load_sem, send_sem, aside_sem, recv_sem, stats_sem,
):
    rows = kv.shape[2] // 2
    tall = per_group * HEAD_SIZE
    wide = per_group * rows
    me = lax.axis_index("seq")
    phase = lax.rem(lax.axis_index("batch"), 2)
    last, helper = n - 1, n - 2

    def kv_load(g):
        cols = pl.ds(g * HEAD_SIZE, HEAD_SIZE)
        return (
            pltpu.make_async_copy(
                k_hbm.at[0, :, cols], kv.at[0, g, pl.ds(0, rows)], load_sem.at[0]
            ),
            pltpu.make_async_copy(
                v_hbm.at[0, :, cols], kv.at[0, g, pl.ds(rows, rows)], load_sem.at[0]
            ),
        )

    def q_load(g):
        cols = pl.ds(g * tall, tall)
        return pltpu.make_async_copy(q_hbm.at[0, :, cols], q.at[g], load_sem.at[1])

    scripts = {(r, p): script(n, groups, p, r) for r in range(n) for p in range(2)}
    here = {key: (me == key[0]) & (phase == key[1]) for key in scripts}

    def wait_for(ref, sem):
        pltpu.make_async_copy(ref, ref, sem).wait()

    def send(slot, g, nth):
        return pltpu.make_async_remote_copy(
            src_ref=kv.at[slot, g],
            dst_ref=kv.at[slot + 1, g],
            send_sem=send_sem.at[0],
            recv_sem=recv_sem.at[nth],
            device_id={"seq": jnp.minimum(me + 1, last)},
            device_id_type=MESH,
        )

    def arrived(ref, nth):
        pltpu.make_async_copy(ref, ref, recv_sem.at[nth]).wait()

    asked_at = scripts[helper, 0][2]
    given_at = jnp.where(phase == 0, scripts[last, 0][2], scripts[last, 1][2])

    def ask(g):
        return pltpu.make_async_remote_copy(
            src_ref=q.at[g],
            dst_ref=q.at[groups + g],
            send_sem=aside_sem.at[0],
            recv_sem=recv_sem.at[asked_at + g],
            device_id={"seq": jnp.int32(helper)},
            device_id_type=MESH,
        )

    def give(g):
        return (
            pltpu.make_async_remote_copy(
                src_ref=mine.at[g],
                dst_ref=back.at[g],
                send_sem=aside_sem.at[0],
                recv_sem=recv_sem.at[given_at + g],
                device_id={"seq": jnp.int32(last)},
                device_id_type=MESH,
            ),
            pltpu.make_async_remote_copy(
                src_ref=mine_stats.at[g],
                dst_ref=back_stats.at[g],
                send_sem=aside_sem.at[1],
                recv_sem=stats_sem.at[g],
                device_id={"seq": jnp.int32(last)},
                device_id_type=MESH,
            ),
        )

    barrier = pltpu.get_barrier_semaphore()

    @pl.when(me > 0)
    def _():
        pl.semaphore_signal(barrier, inc=1, device_id={"seq": me - 1}, device_id_type=MESH)

    if most:
        @pl.when(me == helper)
        def _():
            pl.semaphore_signal(barrier, inc=1, device_id={"seq": jnp.int32(last)}, device_id_type=MESH)

    for g in range(groups):
        for copy in kv_load(g):
            copy.start()
    for g in range(groups):
        q_load(g).start()

    def pick(values):
        out = jnp.int32(0)
        for key, value in values.items():
            if value:
                out = jnp.where(here[key], jnp.int32(value), out)
        return out

    count = pick({key: len(steps) for key, (_, steps, _) in scripts.items()})
    longest = max(len(steps) for _, steps, _ in scripts.values())
    words = []
    for at in range(0, longest, 2):
        pairs = {key: (steps[at : at + 2] + [0, 0])[:2] for key, (_, steps, _) in scripts.items()}
        words.append(pick({key: low + CODE * high for key, (low, high) in pairs.items()}))

    @pl.when(me < last if not most else me >= 0)
    def _():
        pl.semaphore_wait(barrier, 1)

    wait_for(kv.at[0], load_sem.at[0])

    for (rank, p), (before, _, _) in scripts.items():
        @pl.when(here[rank, p])
        def _(before=before):
            for i, g in enumerate(before):
                send(0, g, i).start()

    wait_for(q.at[pl.ds(0, groups)], load_sem.at[1])

    for p in range(2):
        for g in range(moved_heads(n, groups, p)):
            @pl.when(here[last, p])
            def _(g=g):
                ask(g).start()

    sent_before = pick({key: len(before) for key, (before, _, _) in scripts.items()})

    def scores_of(slot, g, turned):
        return jnp.dot(kv[slot, g, :rows, :], turned, preferred_element_type=jnp.float32)

    def weighted(p, slot, g):
        return jnp.dot(
            kv[slot, g, rows:, :].T, p.astype(jnp.bfloat16), preferred_element_type=jnp.float32
        )

    def write(total, g):
        done = total.astype(jnp.bfloat16)
        for h in range(per_group):
            at = pl.multiple_of((g * per_group + h) * HEAD_SIZE, HEAD_SIZE)
            o[0, :, pl.ds(at, HEAD_SIZE)] = done[:, h * rows : (h + 1) * rows].T

    def conclude(qi, g, flag):
        @pl.when(flag == FINISH)
        def _():
            write(acc[qi] * (1.0 / l[qi]), g)

        if most:
            @pl.when(flag == RETURN)
            def _():
                mine[g] = (acc[qi] * (1.0 / l[qi])).astype(jnp.bfloat16)
                mine_stats[g, 0:1] = m[qi]
                mine_stats[g, 1:2] = l[qi]
                for copy in give(g):
                    copy.start()

    key = lax.broadcasted_iota(jnp.int32, (rows, wide), 0)
    query = lax.rem(lax.broadcasted_iota(jnp.int32, (rows, wide), 1), rows)

    def step(i, counts):
        got, sent = counts
        at = jnp.maximum(i - groups, 0)
        word = words[0] if words else jnp.int32(0)
        for j, other in enumerate(words[1:]):
            word = jnp.where(at >= 2 * (j + 1), other, word)
        code = jnp.where(lax.rem(at, 2) == 0, lax.rem(word, CODE), lax.div(word, CODE))
        own = pack(FIRST, 0, 0) + jnp.where(me == 0, pack(FIRST, 0, 0, flag=FINISH), 0) + pack(FIRST, 0, 1) * i
        code = jnp.where(i < groups, own, code)
        op = lax.rem(code, 4)
        slot = lax.rem(lax.div(code, 4), 4)
        g = lax.rem(lax.div(code, 16), 4)
        answer = lax.rem(lax.div(code, 64), 2)
        wait = lax.rem(lax.div(code, 128), 2)
        forward = lax.rem(lax.div(code, 256), 2)
        then = lax.rem(lax.div(code, 512), 8)
        flag = lax.div(code, 4096)
        qi = g + groups * answer

        @pl.when(wait == 1)
        def _():
            arrived(kv.at[slot, g], got)

            @pl.when(forward == 1)
            def _():
                send(slot, g, sent).start()

        sent = sent + forward

        @pl.when(then > 0)
        def _():
            send(0, then - 1, sent).start()

        if most:
            @pl.when((op == FIRST) & (answer == 1))
            def _():
                arrived(q.at[groups + g], asked_at + g)

        @pl.when(op == FIRST)
        def _():
            for h in range(per_group):
                qt[qi, :, h * rows : (h + 1) * rows] = q[qi, :, h * HEAD_SIZE : (h + 1) * HEAD_SIZE].T
            s = jnp.where(key <= query + rows * answer, scores_of(0, g, qt[qi]), -1e30)
            new_m = jnp.max(s, axis=0, keepdims=True)
            p = jnp.exp2((s - new_m) * SCALE)
            m[qi] = new_m
            l[qi] = jnp.sum(p, axis=0, keepdims=True)
            acc[qi] = weighted(p, 0, g)
            conclude(qi, g, flag)

        @pl.when(op == NEXT)
        def _():
            s = scores_of(slot, g, qt[qi])
            old_m = m[qi]
            new_m = jnp.maximum(old_m, jnp.max(s, axis=0, keepdims=True))
            fade = jnp.exp2((old_m - new_m) * SCALE)
            p = jnp.exp2((s - new_m) * SCALE)
            m[qi] = new_m
            l[qi] = l[qi] * fade + jnp.sum(p, axis=0, keepdims=True)
            acc[qi] = acc[qi] * fade + weighted(p, slot, g)
            conclude(qi, g, flag)

        if most:
            @pl.when(op == MERGE)
            def _():
                arrived(back.at[g], given_at + g)
                wait_for(back_stats.at[g], stats_sem.at[g])
                here, there = m[g], back_stats[g, 0:1]
                new_m = jnp.maximum(here, there)
                fade = jnp.exp2((here - new_m) * SCALE)
                weight = jnp.exp2((there - new_m) * SCALE) * back_stats[g, 1:2]
                share = 1.0 / (l[g] * fade + weight)
                write(acc[g] * (fade * share) + back[g].astype(jnp.float32) * (weight * share), g)

        return got + wait, sent + jnp.where(then > 0, 1, 0)

    lax.fori_loop(0, groups + count, step, (jnp.int32(0), sent_before))

    for (rank, p) in scripts:
        away = moved_heads(n, groups, p)

        @pl.when(here[rank, p])
        def _(rank=rank, away=away):
            if rank < helper:
                wait_for(kv.at[pl.ds(0, rank + 1)], send_sem.at[0])
            elif rank == helper:
                wait_for(kv.at[pl.ds(0, rank + 1), pl.ds(away, groups - away)], send_sem.at[0])
                if away:
                    wait_for(mine.at[pl.ds(0, away)], aside_sem.at[0])
                    wait_for(mine_stats.at[pl.ds(0, away)], aside_sem.at[1])
            elif away:
                wait_for(q.at[pl.ds(0, away)], aside_sem.at[0])


def scheduled(n, queries, keys, values):
    rows, query_width = queries.shape[1:]
    groups = keys.shape[2] // HEAD_SIZE
    per_group = query_width // HEAD_SIZE // groups
    tall, wide = per_group * HEAD_SIZE, per_group * rows
    most = max(moved_heads(n, groups, p) for p in range(2))
    held = max(most, 1)
    hbm = pl.BlockSpec(memory_space=pltpu.HBM)
    total = groups + most
    received = max(
        script(n, groups, p, r)[2] + (moved_heads(n, groups, p) if r >= n - 2 else 0)
        for p in range(2)
        for r in range(n)
    )
    bytes_held = (
        2 * rows * query_width * 2
        + total * rows * tall * (2 + 2 + 4)
        + 2 * n * rows * keys.shape[2] * 2
        + 2 * held * rows * tall * 2
        + (2 * total + 4 * held) * 8 * wide * 4
    )
    return pl.pallas_call(
        functools.partial(scheduled_kernel, n, groups, per_group, most),
        out_shape=jax.ShapeDtypeStruct(queries.shape, queries.dtype),
        in_specs=[hbm, hbm, hbm],
        out_specs=pl.BlockSpec(memory_space=pltpu.VMEM),
        scratch_shapes=[
            pltpu.VMEM((total, rows, tall), jnp.bfloat16),
            pltpu.VMEM((total, HEAD_SIZE, wide), jnp.bfloat16),
            pltpu.VMEM((n, groups, 2 * rows, HEAD_SIZE), jnp.bfloat16),
            pltpu.VMEM((total, 1, wide), jnp.float32),
            pltpu.VMEM((total, 1, wide), jnp.float32),
            pltpu.VMEM((total, HEAD_SIZE, wide), jnp.float32),
            pltpu.VMEM((held, HEAD_SIZE, wide), jnp.bfloat16),
            pltpu.VMEM((held, 2, wide), jnp.float32),
            pltpu.VMEM((held, HEAD_SIZE, wide), jnp.bfloat16),
            pltpu.VMEM((held, 2, wide), jnp.float32),
            pltpu.SemaphoreType.DMA((2,)),
            pltpu.SemaphoreType.DMA((1,)),
            pltpu.SemaphoreType.DMA((2,)),
            pltpu.SemaphoreType.DMA((received,)),
            pltpu.SemaphoreType.DMA((held,)),
        ],
        compiler_params=pltpu.CompilerParams(
            collective_id=0, has_side_effects=True, vmem_limit_bytes=bytes_held + 4 * 2**20
        ),
    )(*(pltpu.with_memory_space_constraint(x, pltpu.HBM) for x in (queries, keys, values)))


def kernel(
    n, groups, per_group,
    q_hbm, k_hbm, v_hbm, o,
    q, kv, m, acc,
    load_sem, q_sem, send_sem, recv_sem,
):
    rows = q.shape[0]
    me = lax.axis_index("seq")
    right, left = lax.rem(me + 1, n), lax.rem(me + n - 1, n)

    def loads(g):
        cols = pl.ds(g * HEAD_SIZE, HEAD_SIZE)
        return (
            pltpu.make_async_copy(
                k_hbm.at[0, :, cols], kv.at[0, g, pl.ds(0, rows)], load_sem.at[0, g]
            ),
            pltpu.make_async_copy(
                v_hbm.at[0, :, cols], kv.at[0, g, pl.ds(rows, rows)], load_sem.at[1, g]
            ),
        )

    def send(slot, g):
        return pltpu.make_async_remote_copy(
            src_ref=kv.at[slot, g],
            dst_ref=kv.at[slot + 1, g],
            send_sem=send_sem.at[slot, g],
            recv_sem=recv_sem.at[slot + 1, g],
            device_id={"seq": right},
            device_id_type=MESH,
        )

    def receive(slot, g):
        return pltpu.make_async_remote_copy(
            src_ref=kv.at[slot, g],
            dst_ref=kv.at[slot, g],
            send_sem=send_sem.at[slot, g],
            recv_sem=recv_sem.at[slot, g],
            device_id={"seq": right},
            device_id_type=MESH,
        )

    q_copy = pltpu.make_async_copy(q_hbm.at[0], q, q_sem)

    barrier = pltpu.get_barrier_semaphore()

    @pl.when(me > 0)
    def _():
        pl.semaphore_signal(barrier, inc=1, device_id={"seq": left}, device_id_type=MESH)

    for g in range(groups):
        for copy in loads(g):
            copy.start()
    q_copy.start()

    @pl.when(me < n - 1)
    def _():
        pl.semaphore_wait(barrier, 1)

    for g in range(groups):
        for copy in loads(g):
            copy.wait()

        @pl.when(me < n - 1)
        def _():
            send(0, g).start()

    q_copy.wait()

    def scores_of(slot, g):
        stacked = jnp.concatenate(
            [
                q[:, (g * per_group + h) * HEAD_SIZE : (g * per_group + h + 1) * HEAD_SIZE]
                for h in range(per_group)
            ],
            axis=0,
        )
        return lax.dot_general(
            stacked,
            kv[slot, g, :rows, :],
            (((1,), (1,)), ((), ())),
            preferred_element_type=jnp.float32,
        )

    def weighted(p, slot, g):
        block = jnp.concatenate(
            [kv[slot, g, rows:, :], jnp.ones((rows, HEAD_SIZE), jnp.bfloat16)], axis=1
        )
        return jnp.dot(p.astype(jnp.bfloat16), block, preferred_element_type=jnp.float32)

    def finish(total, g):
        done = (total[:, :HEAD_SIZE] / total[:, HEAD_SIZE:]).astype(jnp.bfloat16)
        for h in range(per_group):
            at = (g * per_group + h) * HEAD_SIZE
            o[0, :, at : at + HEAD_SIZE] = done[h * rows : (h + 1) * rows]

    row = lax.rem(lax.broadcasted_iota(jnp.int32, (per_group * rows, rows), 0), rows)
    visible = lax.broadcasted_iota(jnp.int32, (per_group * rows, rows), 1) <= row

    for g in range(groups):
        s = jnp.where(visible, scores_of(0, g), -1e30)
        new_m = jnp.max(s, axis=1, keepdims=True)
        total = weighted(jnp.exp2((s - new_m) * SCALE), 0, g)
        acc[g] = total
        m[g] = jnp.broadcast_to(new_m, m.shape[1:])

        @pl.when(me == 0)
        def _():
            finish(acc[g], g)

    @pl.loop(1, me + 1)
    def _(slot):
        for g in range(groups):
            receive(slot, g).wait_recv()

            @pl.when(me < n - 1)
            def _():
                send(slot, g).start()

            s = scores_of(slot, g)
            old_m = m[g]
            new_m = jnp.maximum(old_m, jnp.max(s, axis=1, keepdims=True))
            fade = jnp.exp2((old_m - new_m) * SCALE)
            p = jnp.exp2((s - new_m[:, :1]) * SCALE)
            total = acc[g] * jnp.concatenate([fade, fade], axis=1) + weighted(p, slot, g)

            @pl.when(slot < me)
            def _():
                acc[g] = total
                m[g] = new_m

            @pl.when(slot == me)
            def _():
                finish(total, g)

    @pl.when(me < n - 1)
    def _():
        @pl.loop(0, me + 1)
        def _(slot):
            for g in range(groups):
                send(slot, g).wait_send()


def on_device(n, queries, keys, values):
    rows, query_width = queries.shape[1:]
    groups = keys.shape[2] // HEAD_SIZE
    per_group = query_width // HEAD_SIZE // groups
    hbm = pl.BlockSpec(memory_space=pltpu.HBM)
    held = (2 * rows * query_width + 2 * n * rows * keys.shape[2]) * 2 + 3 * rows * query_width * 4
    return pl.pallas_call(
        functools.partial(kernel, n, groups, per_group),
        out_shape=jax.ShapeDtypeStruct(queries.shape, queries.dtype),
        in_specs=[hbm, hbm, hbm],
        out_specs=pl.BlockSpec(memory_space=pltpu.VMEM),
        scratch_shapes=[
            pltpu.VMEM((rows, query_width), jnp.bfloat16),
            pltpu.VMEM((n, groups, 2 * rows, HEAD_SIZE), jnp.bfloat16),
            pltpu.VMEM((groups, per_group * rows, HEAD_SIZE), jnp.float32),
            pltpu.VMEM((groups, per_group * rows, 2 * HEAD_SIZE), jnp.float32),
            pltpu.SemaphoreType.DMA((2, groups)),
            pltpu.SemaphoreType.DMA,
            pltpu.SemaphoreType.DMA((n, groups)),
            pltpu.SemaphoreType.DMA((n, groups)),
        ],
        compiler_params=pltpu.CompilerParams(collective_id=0, has_side_effects=True, vmem_limit_bytes=held + 4 * 2**20),
    )(*(pltpu.with_memory_space_constraint(x, pltpu.HBM) for x in (queries, keys, values)))


def solution(mesh):
    spec = P(("groups", "batch"), "seq", None)
    n = mesh.shape["seq"]
    return jax.shard_map(
        functools.partial(scheduled if n <= SCHEDULED else on_device, n),
        mesh=mesh,
        in_specs=(spec, spec, spec),
        out_specs=spec,
        check_vma=False,
    )
```

```python
import functools
import math

import jax
import jax.numpy as jnp
from jax import lax
from jax.experimental import pallas as pl
from jax.experimental.pallas import tpu as pltpu
from jax.sharding import PartitionSpec as P

HEAD_SIZE = 128
SCALE = math.log2(math.e) / math.sqrt(HEAD_SIZE)
MESH = pl.DeviceIdType.MESH

SCHEDULED = 4

FIRST, NEXT, MERGE, REST = range(4)
KEEP, FINISH, RETURN = range(3)
CODE = 2**14


def pack(op, slot, g, answer=0, wait=0, forward=0, then=0, flag=KEEP):
    code = 0
    for value, size in ((flag, 4), (then, 8), (forward, 2), (wait, 2), (answer, 2), (g, 4), (slot, 4), (op, 4)):
        code = code * size + value
    return code


def moved_heads(n, groups, phase):
    return 0 if n < 4 else groups // (4 if phase == 0 else 2)


def order_of(top, groups, moved, phase):
    stay = list(range(moved, groups))
    own = [(top, g) for g in stay]
    older = [(b, g) for b in range(top - 1, -1, -1) for g in stay]
    away = [(b, g) for g in range(moved) for b in range(top, -1, -1)]
    return own + older + away if phase == 0 else own + away + older


def taken_up(phase, g):
    return 2 + 2 * g


def script(n, groups, phase, rank):
    moved = moved_heads(n, groups, phase)
    helper, last = n - 2, n - 1
    order = order_of(max(n - 3, 0), groups, moved, phase)

    def sends(r):
        mine = [(b, g) for b, g in order if b <= r]
        if r < helper:
            return mine
        own = [(r, g) for g in range(moved, groups)]
        return own + [(b, g) for b, g in mine if g >= moved]

    queue = sends(rank) if rank < last else []
    arrivals = sends(helper) if rank == last else [(b, g) for b, g in order if b < rank]
    before = []
    while queue and queue[0][0] == rank:
        before.append(queue.pop(0)[1])

    steps = []
    left = {g: rank for g in range(groups)}
    waiting = {g: rank for g in range(moved)} if rank == helper else {}
    seen = {g: [] for g in waiting}
    ready = set()
    returned = 0

    def start_answer(g):
        ready.add(g)
        steps.append(pack(FIRST, 0, g, answer=1))
        for slot in seen[g]:
            steps.append(pack(NEXT, slot, g, answer=1))

    for i, (b, g) in enumerate(arrivals):
        slot = rank - b
        how = dict(wait=1)
        if queue and queue[0] == (b, g):
            queue.pop(0)
            how["forward"] = 1
            while queue and queue[0][0] == rank:
                if "then" in how:
                    steps.append(pack(REST, slot, g, **how))
                    how = {}
                how["then"] = queue.pop(0)[1] + 1
        left[g] -= 1
        if g in waiting:
            waiting[g] -= 1
            if g in ready:
                steps.append(pack(NEXT, slot, g, answer=1, flag=KEEP if waiting[g] else RETURN, **how))
                how = {}
            seen[g].append(slot)
        ends = left[g] == 0 and not (rank == last and g < moved)
        steps.append(pack(NEXT, slot, g, flag=FINISH if ends else KEEP, **how))
        for h in waiting:
            due = i + 1 < len(arrivals) and arrivals[i + 1][1] == h and waiting[h] == 1
            if h not in ready and (due or i >= taken_up(phase, h)):
                start_answer(h)
        if rank == last:
            while returned < moved and returns_before(order, moved, returned, groups) <= i + 1:
                steps.append(pack(MERGE, 0, returned))
                returned += 1
    if rank == last:
        steps += [pack(MERGE, 0, g) for g in range(returned, moved)]
    assert not queue
    return before, steps, len(arrivals)


def returns_before(order, moved, g, groups):
    at = max(i for i, (_, h) in enumerate(order) if h == g)
    return groups - moved + sum(1 for _, h in order[:at] if h >= moved)


def scheduled_kernel(
    n, groups, per_group, most,
    q_hbm, k_hbm, v_hbm, o,
    q, qt, kv, m, l, acc, back, back_stats, mine, mine_stats,
    load_sem, send_sem, aside_sem, recv_sem, stats_sem,
):
    rows = kv.shape[2] // 2
    tall = per_group * HEAD_SIZE
    wide = per_group * rows
    me = lax.axis_index("seq")
    phase = lax.rem(lax.axis_index("batch"), 2)
    last, helper = n - 1, n - 2

    def kv_load(g):
        cols = pl.ds(g * HEAD_SIZE, HEAD_SIZE)
        return (
            pltpu.make_async_copy(
                k_hbm.at[0, :, cols], kv.at[0, g, pl.ds(0, rows)], load_sem.at[0]
            ),
            pltpu.make_async_copy(
                v_hbm.at[0, :, cols], kv.at[0, g, pl.ds(rows, rows)], load_sem.at[0]
            ),
        )

    def q_load(g):
        cols = pl.ds(g * tall, tall)
        return pltpu.make_async_copy(q_hbm.at[0, :, cols], q.at[g], load_sem.at[1])

    scripts = {(r, p): script(n, groups, p, r) for r in range(n) for p in range(2)}
    here = {key: (me == key[0]) & (phase == key[1]) for key in scripts}

    def wait_for(ref, sem):
        pltpu.make_async_copy(ref, ref, sem).wait()

    def send(slot, g, nth):
        return pltpu.make_async_remote_copy(
            src_ref=kv.at[slot, g],
            dst_ref=kv.at[slot + 1, g],
            send_sem=send_sem.at[0],
            recv_sem=recv_sem.at[nth],
            device_id={"seq": jnp.minimum(me + 1, last)},
            device_id_type=MESH,
        )

    def arrived(ref, nth):
        pltpu.make_async_copy(ref, ref, recv_sem.at[nth]).wait()

    asked_at = scripts[helper, 0][2]
    given_at = jnp.where(phase == 0, scripts[last, 0][2], scripts[last, 1][2])

    def ask(g):
        return pltpu.make_async_remote_copy(
            src_ref=q.at[g],
            dst_ref=q.at[groups + g],
            send_sem=aside_sem.at[0],
            recv_sem=recv_sem.at[asked_at + g],
            device_id={"seq": jnp.int32(helper)},
            device_id_type=MESH,
        )

    def give(g):
        return (
            pltpu.make_async_remote_copy(
                src_ref=mine.at[g],
                dst_ref=back.at[g],
                send_sem=aside_sem.at[0],
                recv_sem=recv_sem.at[given_at + g],
                device_id={"seq": jnp.int32(last)},
                device_id_type=MESH,
            ),
            pltpu.make_async_remote_copy(
                src_ref=mine_stats.at[g],
                dst_ref=back_stats.at[g],
                send_sem=aside_sem.at[1],
                recv_sem=stats_sem.at[g],
                device_id={"seq": jnp.int32(last)},
                device_id_type=MESH,
            ),
        )

    barrier = pltpu.get_barrier_semaphore()

    @pl.when(me > 0)
    def _():
        pl.semaphore_signal(barrier, inc=1, device_id={"seq": me - 1}, device_id_type=MESH)

    if most:
        @pl.when(me == helper)
        def _():
            pl.semaphore_signal(barrier, inc=1, device_id={"seq": jnp.int32(last)}, device_id_type=MESH)

    for g in range(groups):
        for copy in kv_load(g):
            copy.start()
    for g in range(groups):
        q_load(g).start()

    def pick(values):
        out = jnp.int32(0)
        for key, value in values.items():
            if value:
                out = jnp.where(here[key], jnp.int32(value), out)
        return out

    count = pick({key: len(steps) for key, (_, steps, _) in scripts.items()})
    longest = max(len(steps) for _, steps, _ in scripts.values())
    words = []
    for at in range(0, longest, 2):
        pairs = {key: (steps[at : at + 2] + [0, 0])[:2] for key, (_, steps, _) in scripts.items()}
        words.append(pick({key: low + CODE * high for key, (low, high) in pairs.items()}))

    @pl.when(me < last if not most else me >= 0)
    def _():
        pl.semaphore_wait(barrier, 1)

    wait_for(kv.at[0], load_sem.at[0])

    for (rank, p), (before, _, _) in scripts.items():
        @pl.when(here[rank, p])
        def _(before=before):
            for i, g in enumerate(before):
                send(0, g, i).start()

    wait_for(q.at[pl.ds(0, groups)], load_sem.at[1])

    for p in range(2):
        for g in range(moved_heads(n, groups, p)):
            @pl.when(here[last, p])
            def _(g=g):
                ask(g).start()

    sent_before = pick({key: len(before) for key, (before, _, _) in scripts.items()})

    def scores_of(slot, g, turned):
        return jnp.dot(kv[slot, g, :rows, :], turned, preferred_element_type=jnp.float32)

    def weighted(p, slot, g):
        return jnp.dot(
            kv[slot, g, rows:, :].T, p.astype(jnp.bfloat16), preferred_element_type=jnp.float32
        )

    def write(total, g):
        done = total.astype(jnp.bfloat16)
        for h in range(per_group):
            at = pl.multiple_of((g * per_group + h) * HEAD_SIZE, HEAD_SIZE)
            o[0, :, pl.ds(at, HEAD_SIZE)] = done[:, h * rows : (h + 1) * rows].T

    def conclude(qi, g, flag):
        @pl.when(flag == FINISH)
        def _():
            write(acc[qi] * (1.0 / l[qi]), g)

        if most:
            @pl.when(flag == RETURN)
            def _():
                mine[g] = (acc[qi] * (1.0 / l[qi])).astype(jnp.bfloat16)
                mine_stats[g, 0:1] = m[qi]
                mine_stats[g, 1:2] = l[qi]
                for copy in give(g):
                    copy.start()

    key = lax.broadcasted_iota(jnp.int32, (rows, wide), 0)
    query = lax.rem(lax.broadcasted_iota(jnp.int32, (rows, wide), 1), rows)

    def step(i, counts):
        got, sent = counts
        at = jnp.maximum(i - groups, 0)
        word = words[0] if words else jnp.int32(0)
        for j, other in enumerate(words[1:]):
            word = jnp.where(at >= 2 * (j + 1), other, word)
        code = jnp.where(lax.rem(at, 2) == 0, lax.rem(word, CODE), lax.div(word, CODE))
        own = pack(FIRST, 0, 0) + jnp.where(me == 0, pack(FIRST, 0, 0, flag=FINISH), 0) + pack(FIRST, 0, 1) * i
        code = jnp.where(i < groups, own, code)
        op = lax.rem(code, 4)
        slot = lax.rem(lax.div(code, 4), 4)
        g = lax.rem(lax.div(code, 16), 4)
        answer = lax.rem(lax.div(code, 64), 2)
        wait = lax.rem(lax.div(code, 128), 2)
        forward = lax.rem(lax.div(code, 256), 2)
        then = lax.rem(lax.div(code, 512), 8)
        flag = lax.div(code, 4096)
        qi = g + groups * answer

        @pl.when(wait == 1)
        def _():
            arrived(kv.at[slot, g], got)

            @pl.when(forward == 1)
            def _():
                send(slot, g, sent).start()

        sent = sent + forward

        @pl.when(then > 0)
        def _():
            send(0, then - 1, sent).start()

        if most:
            @pl.when((op == FIRST) & (answer == 1))
            def _():
                arrived(q.at[groups + g], asked_at + g)

        @pl.when(op == FIRST)
        def _():
            for h in range(per_group):
                qt[qi, :, h * rows : (h + 1) * rows] = q[qi, :, h * HEAD_SIZE : (h + 1) * HEAD_SIZE].T
            s = jnp.where(key <= query + rows * answer, scores_of(0, g, qt[qi]), -1e30)
            new_m = jnp.max(s, axis=0, keepdims=True)
            p = jnp.exp2((s - new_m) * SCALE)
            m[qi] = new_m
            l[qi] = jnp.sum(p, axis=0, keepdims=True)
            acc[qi] = weighted(p, 0, g)
            conclude(qi, g, flag)

        @pl.when(op == NEXT)
        def _():
            s = scores_of(slot, g, qt[qi])
            old_m = m[qi]
            new_m = jnp.maximum(old_m, jnp.max(s, axis=0, keepdims=True))
            fade = jnp.exp2((old_m - new_m) * SCALE)
            p = jnp.exp2((s - new_m) * SCALE)
            m[qi] = new_m
            l[qi] = l[qi] * fade + jnp.sum(p, axis=0, keepdims=True)
            acc[qi] = acc[qi] * fade + weighted(p, slot, g)
            conclude(qi, g, flag)

        if most:
            @pl.when(op == MERGE)
            def _():
                arrived(back.at[g], given_at + g)
                wait_for(back_stats.at[g], stats_sem.at[g])
                here, there = m[g], back_stats[g, 0:1]
                new_m = jnp.maximum(here, there)
                fade = jnp.exp2((here - new_m) * SCALE)
                weight = jnp.exp2((there - new_m) * SCALE) * back_stats[g, 1:2]
                share = 1.0 / (l[g] * fade + weight)
                write(acc[g] * (fade * share) + back[g].astype(jnp.float32) * (weight * share), g)

        return got + wait, sent + jnp.where(then > 0, 1, 0)

    lax.fori_loop(0, groups + count, step, (jnp.int32(0), sent_before))

    for (rank, p) in scripts:
        away = moved_heads(n, groups, p)

        @pl.when(here[rank, p])
        def _(rank=rank, away=away):
            if rank < helper:
                wait_for(kv.at[pl.ds(0, rank + 1)], send_sem.at[0])
            elif rank == helper:
                wait_for(kv.at[pl.ds(0, rank + 1), pl.ds(away, groups - away)], send_sem.at[0])
                if away:
                    wait_for(mine.at[pl.ds(0, away)], aside_sem.at[0])
                    wait_for(mine_stats.at[pl.ds(0, away)], aside_sem.at[1])
            elif away:
                wait_for(q.at[pl.ds(0, away)], aside_sem.at[0])


def scheduled(n, queries, keys, values):
    rows, query_width = queries.shape[1:]
    groups = keys.shape[2] // HEAD_SIZE
    per_group = query_width // HEAD_SIZE // groups
    tall, wide = per_group * HEAD_SIZE, per_group * rows
    most = max(moved_heads(n, groups, p) for p in range(2))
    held = max(most, 1)
    hbm = pl.BlockSpec(memory_space=pltpu.HBM)
    total = groups + most
    received = max(
        script(n, groups, p, r)[2] + (moved_heads(n, groups, p) if r >= n - 2 else 0)
        for p in range(2)
        for r in range(n)
    )
    bytes_held = (
        2 * rows * query_width * 2
        + total * rows * tall * (2 + 2 + 4)
        + 2 * n * rows * keys.shape[2] * 2
        + 2 * held * rows * tall * 2
        + (2 * total + 4 * held) * 8 * wide * 4
    )
    return pl.pallas_call(
        functools.partial(scheduled_kernel, n, groups, per_group, most),
        out_shape=jax.ShapeDtypeStruct(queries.shape, queries.dtype),
        in_specs=[hbm, hbm, hbm],
        out_specs=pl.BlockSpec(memory_space=pltpu.VMEM),
        scratch_shapes=[
            pltpu.VMEM((total, rows, tall), jnp.bfloat16),
            pltpu.VMEM((total, HEAD_SIZE, wide), jnp.bfloat16),
            pltpu.VMEM((n, groups, 2 * rows, HEAD_SIZE), jnp.bfloat16),
            pltpu.VMEM((total, 1, wide), jnp.float32),
            pltpu.VMEM((total, 1, wide), jnp.float32),
            pltpu.VMEM((total, HEAD_SIZE, wide), jnp.float32),
            pltpu.VMEM((held, HEAD_SIZE, wide), jnp.bfloat16),
            pltpu.VMEM((held, 2, wide), jnp.float32),
            pltpu.VMEM((held, HEAD_SIZE, wide), jnp.bfloat16),
            pltpu.VMEM((held, 2, wide), jnp.float32),
            pltpu.SemaphoreType.DMA((2,)),
            pltpu.SemaphoreType.DMA((1,)),
            pltpu.SemaphoreType.DMA((2,)),
            pltpu.SemaphoreType.DMA((received,)),
            pltpu.SemaphoreType.DMA((held,)),
        ],
        compiler_params=pltpu.CompilerParams(
            collective_id=0, has_side_effects=True, vmem_limit_bytes=bytes_held + 4 * 2**20
        ),
    )(*(pltpu.with_memory_space_constraint(x, pltpu.HBM) for x in (queries, keys, values)))


def kernel(
    n, groups, per_group,
    q_hbm, k_hbm, v_hbm, o,
    q, kv, m, acc,
    load_sem, q_sem, send_sem, recv_sem,
):
    rows = q.shape[0]
    me = lax.axis_index("seq")
    right, left = lax.rem(me + 1, n), lax.rem(me + n - 1, n)

    def loads(g):
        cols = pl.ds(g * HEAD_SIZE, HEAD_SIZE)
        return (
            pltpu.make_async_copy(
                k_hbm.at[0, :, cols], kv.at[0, g, pl.ds(0, rows)], load_sem.at[0, g]
            ),
            pltpu.make_async_copy(
                v_hbm.at[0, :, cols], kv.at[0, g, pl.ds(rows, rows)], load_sem.at[1, g]
            ),
        )

    def send(slot, g):
        return pltpu.make_async_remote_copy(
            src_ref=kv.at[slot, g],
            dst_ref=kv.at[slot + 1, g],
            send_sem=send_sem.at[slot, g],
            recv_sem=recv_sem.at[slot + 1, g],
            device_id={"seq": right},
            device_id_type=MESH,
        )

    def receive(slot, g):
        return pltpu.make_async_remote_copy(
            src_ref=kv.at[slot, g],
            dst_ref=kv.at[slot, g],
            send_sem=send_sem.at[slot, g],
            recv_sem=recv_sem.at[slot, g],
            device_id={"seq": right},
            device_id_type=MESH,
        )

    q_copy = pltpu.make_async_copy(q_hbm.at[0], q, q_sem)

    barrier = pltpu.get_barrier_semaphore()

    @pl.when(me > 0)
    def _():
        pl.semaphore_signal(barrier, inc=1, device_id={"seq": left}, device_id_type=MESH)

    for g in range(groups):
        for copy in loads(g):
            copy.start()
    q_copy.start()

    @pl.when(me < n - 1)
    def _():
        pl.semaphore_wait(barrier, 1)

    for g in range(groups):
        for copy in loads(g):
            copy.wait()

        @pl.when(me < n - 1)
        def _():
            send(0, g).start()

    q_copy.wait()

    def scores_of(slot, g):
        stacked = jnp.concatenate(
            [
                q[:, (g * per_group + h) * HEAD_SIZE : (g * per_group + h + 1) * HEAD_SIZE]
                for h in range(per_group)
            ],
            axis=0,
        )
        return lax.dot_general(
            stacked,
            kv[slot, g, :rows, :],
            (((1,), (1,)), ((), ())),
            preferred_element_type=jnp.float32,
        )

    def weighted(p, slot, g):
        block = jnp.concatenate(
            [kv[slot, g, rows:, :], jnp.ones((rows, HEAD_SIZE), jnp.bfloat16)], axis=1
        )
        return jnp.dot(p.astype(jnp.bfloat16), block, preferred_element_type=jnp.float32)

    def finish(total, g):
        done = (total[:, :HEAD_SIZE] / total[:, HEAD_SIZE:]).astype(jnp.bfloat16)
        for h in range(per_group):
            at = (g * per_group + h) * HEAD_SIZE
            o[0, :, at : at + HEAD_SIZE] = done[h * rows : (h + 1) * rows]

    row = lax.rem(lax.broadcasted_iota(jnp.int32, (per_group * rows, rows), 0), rows)
    visible = lax.broadcasted_iota(jnp.int32, (per_group * rows, rows), 1) <= row

    for g in range(groups):
        s = jnp.where(visible, scores_of(0, g), -1e30)
        new_m = jnp.max(s, axis=1, keepdims=True)
        total = weighted(jnp.exp2((s - new_m) * SCALE), 0, g)
        acc[g] = total
        m[g] = jnp.broadcast_to(new_m, m.shape[1:])

        @pl.when(me == 0)
        def _():
            finish(acc[g], g)

    @pl.loop(1, me + 1)
    def _(slot):
        for g in range(groups):
            receive(slot, g).wait_recv()

            @pl.when(me < n - 1)
            def _():
                send(slot, g).start()

            s = scores_of(slot, g)
            old_m = m[g]
            new_m = jnp.maximum(old_m, jnp.max(s, axis=1, keepdims=True))
            fade = jnp.exp2((old_m - new_m) * SCALE)
            p = jnp.exp2((s - new_m[:, :1]) * SCALE)
            total = acc[g] * jnp.concatenate([fade, fade], axis=1) + weighted(p, slot, g)

            @pl.when(slot < me)
            def _():
                acc[g] = total
                m[g] = new_m

            @pl.when(slot == me)
            def _():
                finish(total, g)

    @pl.when(me < n - 1)
    def _():
        @pl.loop(0, me + 1)
        def _(slot):
            for g in range(groups):
                send(slot, g).wait_send()


def on_device(n, queries, keys, values):
    rows, query_width = queries.shape[1:]
    groups = keys.shape[2] // HEAD_SIZE
    per_group = query_width // HEAD_SIZE // groups
    hbm = pl.BlockSpec(memory_space=pltpu.HBM)
    held = (2 * rows * query_width + 2 * n * rows * keys.shape[2]) * 2 + 3 * rows * query_width * 4
    return pl.pallas_call(
        functools.partial(kernel, n, groups, per_group),
        out_shape=jax.ShapeDtypeStruct(queries.shape, queries.dtype),
        in_specs=[hbm, hbm, hbm],
        out_specs=pl.BlockSpec(memory_space=pltpu.VMEM),
        scratch_shapes=[
            pltpu.VMEM((rows, query_width), jnp.bfloat16),
            pltpu.VMEM((n, groups, 2 * rows, HEAD_SIZE), jnp.bfloat16),
            pltpu.VMEM((groups, per_group * rows, HEAD_SIZE), jnp.float32),
            pltpu.VMEM((groups, per_group * rows, 2 * HEAD_SIZE), jnp.float32),
            pltpu.SemaphoreType.DMA((2, groups)),
            pltpu.SemaphoreType.DMA,
            pltpu.SemaphoreType.DMA((n, groups)),
            pltpu.SemaphoreType.DMA((n, groups)),
        ],
        compiler_params=pltpu.CompilerParams(collective_id=0, has_side_effects=True, vmem_limit_bytes=held + 4 * 2**20),
    )(*(pltpu.with_memory_space_constraint(x, pltpu.HBM) for x in (queries, keys, values)))


def solution(mesh):
    spec = P(("groups", "batch"), "seq", None)
    n = mesh.shape["seq"]
    return jax.shard_map(
        functools.partial(scheduled if n <= SCHEDULED else on_device, n),
        mesh=mesh,
        in_specs=(spec, spec, spec),
        out_specs=spec,
        check_vma=False,
    )
```

```python
import functools
import math

import jax
import jax.numpy as jnp
from jax import lax
from jax.experimental import pallas as pl
from jax.experimental.pallas import tpu as pltpu
from jax.sharding import PartitionSpec as P

HEAD_SIZE = 128
SCALE = math.log2(math.e) / math.sqrt(HEAD_SIZE)
MESH = pl.DeviceIdType.MESH

SCHEDULED = 4

FIRST, NEXT, MERGE, REST = range(4)
KEEP, FINISH, RETURN = range(3)
CODE = 2**14


def pack(op, slot, g, answer=0, wait=0, forward=0, then=0, flag=KEEP):
    code = 0
    for value, size in ((flag, 4), (then, 8), (forward, 2), (wait, 2), (answer, 2), (g, 4), (slot, 4), (op, 4)):
        code = code * size + value
    return code


def moved_heads(n, groups, phase):
    return 0 if n < 4 else groups // (4 if phase == 0 else 2)


def order_of(top, groups, moved, phase):
    stay = list(range(moved, groups))
    own = [(top, g) for g in stay]
    older = [(b, g) for b in range(top - 1, -1, -1) for g in stay]
    away = [(b, g) for g in range(moved) for b in range(top, -1, -1)]
    return own + older + away if phase == 0 else own + away + older


def taken_up(phase, g):
    return 2 + 2 * g


def script(n, groups, phase, rank):
    moved = moved_heads(n, groups, phase)
    helper, last = n - 2, n - 1
    order = order_of(max(n - 3, 0), groups, moved, phase)

    def sends(r):
        mine = [(b, g) for b, g in order if b <= r]
        if r < helper:
            return mine
        own = [(r, g) for g in range(moved, groups)]
        return own + [(b, g) for b, g in mine if g >= moved]

    queue = sends(rank) if rank < last else []
    arrivals = sends(helper) if rank == last else [(b, g) for b, g in order if b < rank]
    before = []
    while queue and queue[0][0] == rank:
        before.append(queue.pop(0)[1])

    steps = []
    left = {g: rank for g in range(groups)}
    waiting = {g: rank for g in range(moved)} if rank == helper else {}
    seen = {g: [] for g in waiting}
    ready = set()
    returned, later = 0, []

    def start_answer(g):
        ready.add(g)
        steps.append(pack(FIRST, 0, g, answer=1))
        for slot in seen[g]:
            steps.append(pack(NEXT, slot, g, answer=1))

    for i, (b, g) in enumerate(arrivals):
        slot = rank - b
        how = dict(wait=1)
        if queue and queue[0] == (b, g):
            queue.pop(0)
            how["forward"] = 1
            while queue and queue[0][0] == rank:
                if "then" in how:
                    steps.append(pack(REST, slot, g, **how))
                    how = {}
                how["then"] = queue.pop(0)[1] + 1
        left[g] -= 1
        if g in waiting:
            waiting[g] -= 1
            if g in ready:
                steps.append(pack(NEXT, slot, g, answer=1, flag=KEEP if waiting[g] else RETURN, **how))
                how = {}
            seen[g].append(slot)
        ends = left[g] == 0 and not (rank == last and g < moved)
        if g in waiting and waiting[g] and i + 1 < len(arrivals) and arrivals[i + 1][1] == g:
            if how:
                steps.append(pack(REST, slot, g, **how))
            later.append(pack(NEXT, slot, g))
        else:
            steps += later
            steps.append(pack(NEXT, slot, g, flag=FINISH if ends else KEEP, **how))
            later = []
        for h in waiting:
            due = i + 1 < len(arrivals) and arrivals[i + 1][1] == h and waiting[h] == 1
            if h not in ready and (due or i >= taken_up(phase, h)):
                start_answer(h)
        if rank == last:
            while returned < moved and returns_before(order, moved, returned, groups) <= i + 1:
                steps.append(pack(MERGE, 0, returned))
                returned += 1
    if rank == last:
        steps += [pack(MERGE, 0, g) for g in range(returned, moved)]
    assert not queue and not later
    return before, steps, len(arrivals)


def returns_before(order, moved, g, groups):
    at = max(i for i, (_, h) in enumerate(order) if h == g)
    return groups - moved + sum(1 for _, h in order[:at] if h >= moved)


def scheduled_kernel(
    n, groups, per_group, most,
    q_hbm, k_hbm, v_hbm, o,
    q, qt, kv, m, l, acc, back, back_stats, mine, mine_stats,
    load_sem, send_sem, aside_sem, recv_sem, stats_sem,
):
    rows = kv.shape[2] // 2
    tall = per_group * HEAD_SIZE
    wide = per_group * rows
    me = lax.axis_index("seq")
    phase = lax.rem(lax.axis_index("batch"), 2)
    last, helper = n - 1, n - 2

    def kv_load(g):
        cols = pl.ds(g * HEAD_SIZE, HEAD_SIZE)
        return (
            pltpu.make_async_copy(
                k_hbm.at[0, :, cols], kv.at[0, g, pl.ds(0, rows)], load_sem.at[0]
            ),
            pltpu.make_async_copy(
                v_hbm.at[0, :, cols], kv.at[0, g, pl.ds(rows, rows)], load_sem.at[0]
            ),
        )

    def q_load(g):
        cols = pl.ds(g * tall, tall)
        return pltpu.make_async_copy(q_hbm.at[0, :, cols], q.at[g], load_sem.at[1])

    scripts = {(r, p): script(n, groups, p, r) for r in range(n) for p in range(2)}
    here = {key: (me == key[0]) & (phase == key[1]) for key in scripts}

    def wait_for(ref, sem):
        pltpu.make_async_copy(ref, ref, sem).wait()

    def send(slot, g, nth):
        return pltpu.make_async_remote_copy(
            src_ref=kv.at[slot, g],
            dst_ref=kv.at[slot + 1, g],
            send_sem=send_sem.at[0],
            recv_sem=recv_sem.at[nth],
            device_id={"seq": jnp.minimum(me + 1, last)},
            device_id_type=MESH,
        )

    def arrived(ref, nth):
        pltpu.make_async_copy(ref, ref, recv_sem.at[nth]).wait()

    asked_at = scripts[helper, 0][2]
    given_at = jnp.where(phase == 0, scripts[last, 0][2], scripts[last, 1][2])

    def ask(g):
        return pltpu.make_async_remote_copy(
            src_ref=q.at[g],
            dst_ref=q.at[groups + g],
            send_sem=aside_sem.at[0],
            recv_sem=recv_sem.at[asked_at + g],
            device_id={"seq": jnp.int32(helper)},
            device_id_type=MESH,
        )

    def give(g):
        return (
            pltpu.make_async_remote_copy(
                src_ref=mine.at[g],
                dst_ref=back.at[g],
                send_sem=aside_sem.at[0],
                recv_sem=recv_sem.at[given_at + g],
                device_id={"seq": jnp.int32(last)},
                device_id_type=MESH,
            ),
            pltpu.make_async_remote_copy(
                src_ref=mine_stats.at[g],
                dst_ref=back_stats.at[g],
                send_sem=aside_sem.at[1],
                recv_sem=stats_sem.at[g],
                device_id={"seq": jnp.int32(last)},
                device_id_type=MESH,
            ),
        )

    barrier = pltpu.get_barrier_semaphore()

    @pl.when(me > 0)
    def _():
        pl.semaphore_signal(barrier, inc=1, device_id={"seq": me - 1}, device_id_type=MESH)

    if most:
        @pl.when(me == helper)
        def _():
            pl.semaphore_signal(barrier, inc=1, device_id={"seq": jnp.int32(last)}, device_id_type=MESH)

    for g in range(groups):
        for copy in kv_load(g):
            copy.start()
    for g in range(groups):
        q_load(g).start()

    def pick(values):
        out = jnp.int32(0)
        for key, value in values.items():
            if value:
                out = jnp.where(here[key], jnp.int32(value), out)
        return out

    count = pick({key: len(steps) for key, (_, steps, _) in scripts.items()})
    longest = max(len(steps) for _, steps, _ in scripts.values())
    words = []
    for at in range(0, longest, 2):
        pairs = {key: (steps[at : at + 2] + [0, 0])[:2] for key, (_, steps, _) in scripts.items()}
        words.append(pick({key: low + CODE * high for key, (low, high) in pairs.items()}))

    @pl.when(me < last if not most else me >= 0)
    def _():
        pl.semaphore_wait(barrier, 1)

    wait_for(kv.at[0], load_sem.at[0])

    for (rank, p), (before, _, _) in scripts.items():
        @pl.when(here[rank, p])
        def _(before=before):
            for i, g in enumerate(before):
                send(0, g, i).start()

    wait_for(q.at[pl.ds(0, groups)], load_sem.at[1])

    for p in range(2):
        for g in range(moved_heads(n, groups, p)):
            @pl.when(here[last, p])
            def _(g=g):
                ask(g).start()

    sent_before = pick({key: len(before) for key, (before, _, _) in scripts.items()})

    def scores_of(slot, g, turned):
        return jnp.dot(kv[slot, g, :rows, :], turned, preferred_element_type=jnp.float32)

    def weighted(p, slot, g):
        return jnp.dot(
            kv[slot, g, rows:, :].T, p.astype(jnp.bfloat16), preferred_element_type=jnp.float32
        )

    def write(total, g):
        done = total.astype(jnp.bfloat16)
        for h in range(per_group):
            at = pl.multiple_of((g * per_group + h) * HEAD_SIZE, HEAD_SIZE)
            o[0, :, pl.ds(at, HEAD_SIZE)] = done[:, h * rows : (h + 1) * rows].T

    def conclude(qi, g, flag):
        @pl.when(flag == FINISH)
        def _():
            write(acc[qi] * (1.0 / l[qi]), g)

        if most:
            @pl.when(flag == RETURN)
            def _():
                mine[g] = (acc[qi] * (1.0 / l[qi])).astype(jnp.bfloat16)
                mine_stats[g, 0:1] = m[qi]
                mine_stats[g, 1:2] = l[qi]
                for copy in give(g):
                    copy.start()

    key = lax.broadcasted_iota(jnp.int32, (rows, wide), 0)
    query = lax.rem(lax.broadcasted_iota(jnp.int32, (rows, wide), 1), rows)

    def step(i, counts):
        got, sent = counts
        at = jnp.maximum(i - groups, 0)
        word = words[0] if words else jnp.int32(0)
        for j, other in enumerate(words[1:]):
            word = jnp.where(at >= 2 * (j + 1), other, word)
        code = jnp.where(lax.rem(at, 2) == 0, lax.rem(word, CODE), lax.div(word, CODE))
        own = pack(FIRST, 0, 0) + jnp.where(me == 0, pack(FIRST, 0, 0, flag=FINISH), 0) + pack(FIRST, 0, 1) * i
        code = jnp.where(i < groups, own, code)
        op = lax.rem(code, 4)
        slot = lax.rem(lax.div(code, 4), 4)
        g = lax.rem(lax.div(code, 16), 4)
        answer = lax.rem(lax.div(code, 64), 2)
        wait = lax.rem(lax.div(code, 128), 2)
        forward = lax.rem(lax.div(code, 256), 2)
        then = lax.rem(lax.div(code, 512), 8)
        flag = lax.div(code, 4096)
        qi = g + groups * answer

        @pl.when(wait == 1)
        def _():
            arrived(kv.at[slot, g], got)

            @pl.when(forward == 1)
            def _():
                send(slot, g, sent).start()

        sent = sent + forward

        @pl.when(then > 0)
        def _():
            send(0, then - 1, sent).start()

        if most:
            @pl.when((op == FIRST) & (answer == 1))
            def _():
                arrived(q.at[groups + g], asked_at + g)

        @pl.when(op == FIRST)
        def _():
            for h in range(per_group):
                qt[qi, :, h * rows : (h + 1) * rows] = q[qi, :, h * HEAD_SIZE : (h + 1) * HEAD_SIZE].T
            s = jnp.where(key <= query + rows * answer, scores_of(0, g, qt[qi]), -1e30)
            new_m = jnp.max(s, axis=0, keepdims=True)
            p = jnp.exp2((s - new_m) * SCALE)
            m[qi] = new_m
            l[qi] = jnp.sum(p, axis=0, keepdims=True)
            acc[qi] = weighted(p, 0, g)
            conclude(qi, g, flag)

        @pl.when(op == NEXT)
        def _():
            s = scores_of(slot, g, qt[qi])
            old_m = m[qi]
            new_m = jnp.maximum(old_m, jnp.max(s, axis=0, keepdims=True))
            fade = jnp.exp2((old_m - new_m) * SCALE)
            p = jnp.exp2((s - new_m) * SCALE)
            m[qi] = new_m
            l[qi] = l[qi] * fade + jnp.sum(p, axis=0, keepdims=True)
            acc[qi] = acc[qi] * fade + weighted(p, slot, g)
            conclude(qi, g, flag)

        if most:
            @pl.when(op == MERGE)
            def _():
                arrived(back.at[g], given_at + g)
                wait_for(back_stats.at[g], stats_sem.at[g])
                here, there = m[g], back_stats[g, 0:1]
                new_m = jnp.maximum(here, there)
                fade = jnp.exp2((here - new_m) * SCALE)
                weight = jnp.exp2((there - new_m) * SCALE) * back_stats[g, 1:2]
                share = 1.0 / (l[g] * fade + weight)
                write(acc[g] * (fade * share) + back[g].astype(jnp.float32) * (weight * share), g)

        return got + wait, sent + jnp.where(then > 0, 1, 0)

    lax.fori_loop(0, groups + count, step, (jnp.int32(0), sent_before))

    for (rank, p) in scripts:
        away = moved_heads(n, groups, p)

        @pl.when(here[rank, p])
        def _(rank=rank, away=away):
            if rank < helper:
                wait_for(kv.at[pl.ds(0, rank + 1)], send_sem.at[0])
            elif rank == helper:
                wait_for(kv.at[pl.ds(0, rank + 1), pl.ds(away, groups - away)], send_sem.at[0])
                if away:
                    wait_for(mine.at[pl.ds(0, away)], aside_sem.at[0])
                    wait_for(mine_stats.at[pl.ds(0, away)], aside_sem.at[1])
            elif away:
                wait_for(q.at[pl.ds(0, away)], aside_sem.at[0])


def scheduled(n, queries, keys, values):
    rows, query_width = queries.shape[1:]
    groups = keys.shape[2] // HEAD_SIZE
    per_group = query_width // HEAD_SIZE // groups
    tall, wide = per_group * HEAD_SIZE, per_group * rows
    most = max(moved_heads(n, groups, p) for p in range(2))
    held = max(most, 1)
    hbm = pl.BlockSpec(memory_space=pltpu.HBM)
    total = groups + most
    received = max(
        script(n, groups, p, r)[2] + (moved_heads(n, groups, p) if r >= n - 2 else 0)
        for p in range(2)
        for r in range(n)
    )
    bytes_held = (
        2 * rows * query_width * 2
        + total * rows * tall * (2 + 2 + 4)
        + 2 * n * rows * keys.shape[2] * 2
        + 2 * held * rows * tall * 2
        + (2 * total + 4 * held) * 8 * wide * 4
    )
    return pl.pallas_call(
        functools.partial(scheduled_kernel, n, groups, per_group, most),
        out_shape=jax.ShapeDtypeStruct(queries.shape, queries.dtype),
        in_specs=[hbm, hbm, hbm],
        out_specs=pl.BlockSpec(memory_space=pltpu.VMEM),
        scratch_shapes=[
            pltpu.VMEM((total, rows, tall), jnp.bfloat16),
            pltpu.VMEM((total, HEAD_SIZE, wide), jnp.bfloat16),
            pltpu.VMEM((n, groups, 2 * rows, HEAD_SIZE), jnp.bfloat16),
            pltpu.VMEM((total, 1, wide), jnp.float32),
            pltpu.VMEM((total, 1, wide), jnp.float32),
            pltpu.VMEM((total, HEAD_SIZE, wide), jnp.float32),
            pltpu.VMEM((held, HEAD_SIZE, wide), jnp.bfloat16),
            pltpu.VMEM((held, 2, wide), jnp.float32),
            pltpu.VMEM((held, HEAD_SIZE, wide), jnp.bfloat16),
            pltpu.VMEM((held, 2, wide), jnp.float32),
            pltpu.SemaphoreType.DMA((2,)),
            pltpu.SemaphoreType.DMA((1,)),
            pltpu.SemaphoreType.DMA((2,)),
            pltpu.SemaphoreType.DMA((received,)),
            pltpu.SemaphoreType.DMA((held,)),
        ],
        compiler_params=pltpu.CompilerParams(
            collective_id=0, has_side_effects=True, vmem_limit_bytes=bytes_held + 4 * 2**20
        ),
    )(*(pltpu.with_memory_space_constraint(x, pltpu.HBM) for x in (queries, keys, values)))


def kernel(
    n, groups, per_group,
    q_hbm, k_hbm, v_hbm, o,
    q, kv, m, acc,
    load_sem, q_sem, send_sem, recv_sem,
):
    rows = q.shape[0]
    me = lax.axis_index("seq")
    right, left = lax.rem(me + 1, n), lax.rem(me + n - 1, n)

    def loads(g):
        cols = pl.ds(g * HEAD_SIZE, HEAD_SIZE)
        return (
            pltpu.make_async_copy(
                k_hbm.at[0, :, cols], kv.at[0, g, pl.ds(0, rows)], load_sem.at[0, g]
            ),
            pltpu.make_async_copy(
                v_hbm.at[0, :, cols], kv.at[0, g, pl.ds(rows, rows)], load_sem.at[1, g]
            ),
        )

    def send(slot, g):
        return pltpu.make_async_remote_copy(
            src_ref=kv.at[slot, g],
            dst_ref=kv.at[slot + 1, g],
            send_sem=send_sem.at[slot, g],
            recv_sem=recv_sem.at[slot + 1, g],
            device_id={"seq": right},
            device_id_type=MESH,
        )

    def receive(slot, g):
        return pltpu.make_async_remote_copy(
            src_ref=kv.at[slot, g],
            dst_ref=kv.at[slot, g],
            send_sem=send_sem.at[slot, g],
            recv_sem=recv_sem.at[slot, g],
            device_id={"seq": right},
            device_id_type=MESH,
        )

    q_copy = pltpu.make_async_copy(q_hbm.at[0], q, q_sem)

    barrier = pltpu.get_barrier_semaphore()

    @pl.when(me > 0)
    def _():
        pl.semaphore_signal(barrier, inc=1, device_id={"seq": left}, device_id_type=MESH)

    for g in range(groups):
        for copy in loads(g):
            copy.start()
    q_copy.start()

    @pl.when(me < n - 1)
    def _():
        pl.semaphore_wait(barrier, 1)

    for g in range(groups):
        for copy in loads(g):
            copy.wait()

        @pl.when(me < n - 1)
        def _():
            send(0, g).start()

    q_copy.wait()

    def scores_of(slot, g):
        stacked = jnp.concatenate(
            [
                q[:, (g * per_group + h) * HEAD_SIZE : (g * per_group + h + 1) * HEAD_SIZE]
                for h in range(per_group)
            ],
            axis=0,
        )
        return lax.dot_general(
            stacked,
            kv[slot, g, :rows, :],
            (((1,), (1,)), ((), ())),
            preferred_element_type=jnp.float32,
        )

    def weighted(p, slot, g):
        block = jnp.concatenate(
            [kv[slot, g, rows:, :], jnp.ones((rows, HEAD_SIZE), jnp.bfloat16)], axis=1
        )
        return jnp.dot(p.astype(jnp.bfloat16), block, preferred_element_type=jnp.float32)

    def finish(total, g):
        done = (total[:, :HEAD_SIZE] / total[:, HEAD_SIZE:]).astype(jnp.bfloat16)
        for h in range(per_group):
            at = (g * per_group + h) * HEAD_SIZE
            o[0, :, at : at + HEAD_SIZE] = done[h * rows : (h + 1) * rows]

    row = lax.rem(lax.broadcasted_iota(jnp.int32, (per_group * rows, rows), 0), rows)
    visible = lax.broadcasted_iota(jnp.int32, (per_group * rows, rows), 1) <= row

    for g in range(groups):
        s = jnp.where(visible, scores_of(0, g), -1e30)
        new_m = jnp.max(s, axis=1, keepdims=True)
        total = weighted(jnp.exp2((s - new_m) * SCALE), 0, g)
        acc[g] = total
        m[g] = jnp.broadcast_to(new_m, m.shape[1:])

        @pl.when(me == 0)
        def _():
            finish(acc[g], g)

    @pl.loop(1, me + 1)
    def _(slot):
        for g in range(groups):
            receive(slot, g).wait_recv()

            @pl.when(me < n - 1)
            def _():
                send(slot, g).start()

            s = scores_of(slot, g)
            old_m = m[g]
            new_m = jnp.maximum(old_m, jnp.max(s, axis=1, keepdims=True))
            fade = jnp.exp2((old_m - new_m) * SCALE)
            p = jnp.exp2((s - new_m[:, :1]) * SCALE)
            total = acc[g] * jnp.concatenate([fade, fade], axis=1) + weighted(p, slot, g)

            @pl.when(slot < me)
            def _():
                acc[g] = total
                m[g] = new_m

            @pl.when(slot == me)
            def _():
                finish(total, g)

    @pl.when(me < n - 1)
    def _():
        @pl.loop(0, me + 1)
        def _(slot):
            for g in range(groups):
                send(slot, g).wait_send()


def on_device(n, queries, keys, values):
    rows, query_width = queries.shape[1:]
    groups = keys.shape[2] // HEAD_SIZE
    per_group = query_width // HEAD_SIZE // groups
    hbm = pl.BlockSpec(memory_space=pltpu.HBM)
    held = (2 * rows * query_width + 2 * n * rows * keys.shape[2]) * 2 + 3 * rows * query_width * 4
    return pl.pallas_call(
        functools.partial(kernel, n, groups, per_group),
        out_shape=jax.ShapeDtypeStruct(queries.shape, queries.dtype),
        in_specs=[hbm, hbm, hbm],
        out_specs=pl.BlockSpec(memory_space=pltpu.VMEM),
        scratch_shapes=[
            pltpu.VMEM((rows, query_width), jnp.bfloat16),
            pltpu.VMEM((n, groups, 2 * rows, HEAD_SIZE), jnp.bfloat16),
            pltpu.VMEM((groups, per_group * rows, HEAD_SIZE), jnp.float32),
            pltpu.VMEM((groups, per_group * rows, 2 * HEAD_SIZE), jnp.float32),
            pltpu.SemaphoreType.DMA((2, groups)),
            pltpu.SemaphoreType.DMA,
            pltpu.SemaphoreType.DMA((n, groups)),
            pltpu.SemaphoreType.DMA((n, groups)),
        ],
        compiler_params=pltpu.CompilerParams(collective_id=0, has_side_effects=True, vmem_limit_bytes=held + 4 * 2**20),
    )(*(pltpu.with_memory_space_constraint(x, pltpu.HBM) for x in (queries, keys, values)))


def solution(mesh):
    spec = P(("groups", "batch"), "seq", None)
    n = mesh.shape["seq"]
    return jax.shard_map(
        functools.partial(scheduled if n <= SCHEDULED else on_device, n),
        mesh=mesh,
        in_specs=(spec, spec, spec),
        out_specs=spec,
        check_vma=False,
    )
```

```python
import functools
import math

import jax
import jax.numpy as jnp
from jax import lax
from jax.experimental import pallas as pl
from jax.experimental.pallas import tpu as pltpu
from jax.sharding import PartitionSpec as P

HEAD_SIZE = 128
SCALE = math.log2(math.e) / math.sqrt(HEAD_SIZE)
MESH = pl.DeviceIdType.MESH

SCHEDULED = 4

FIRST, NEXT, MERGE, REST = range(4)
KEEP, FINISH, RETURN = range(3)
CODE = 2**14


def pack(op, slot, g, answer=0, wait=0, forward=0, then=0, flag=KEEP):
    code = 0
    for value, size in ((flag, 4), (then, 8), (forward, 2), (wait, 2), (answer, 2), (g, 4), (slot, 4), (op, 4)):
        code = code * size + value
    return code


def moved_heads(n, groups, phase):
    return 0 if n < 4 else groups // (4 if phase == 0 else 2)


def order_of(top, groups, moved, phase):
    stay = list(range(moved, groups))
    own = [(top, g) for g in stay]
    older = [(b, g) for b in range(top - 1, -1, -1) for g in stay]
    away = [(b, g) for g in range(moved) for b in range(top, -1, -1)]
    return own + older + away if phase == 0 else own + away[: top + 1] + older + away[top + 1 :][::-1]


def taken_up(phase, g):
    return 2 + 2 * g


def script(n, groups, phase, rank):
    moved = moved_heads(n, groups, phase)
    helper, last = n - 2, n - 1
    order = order_of(max(n - 3, 0), groups, moved, phase)

    def sends(r):
        mine = [(b, g) for b, g in order if b <= r]
        if r < helper:
            return mine
        own = [(r, g) for g in range(moved, groups)]
        return own + [(b, g) for b, g in mine if g >= moved]

    queue = sends(rank) if rank < last else []
    arrivals = sends(helper) if rank == last else [(b, g) for b, g in order if b < rank]
    before = []
    while queue and queue[0][0] == rank:
        before.append(queue.pop(0)[1])

    steps = []
    left = {g: rank for g in range(groups)}
    waiting = {g: rank for g in range(moved)} if rank == helper else {}
    seen = {g: [] for g in waiting}
    ready = set()
    returned, later = 0, []

    def start_answer(g):
        ready.add(g)
        steps.append(pack(FIRST, 0, g, answer=1))
        for slot in seen[g]:
            steps.append(pack(NEXT, slot, g, answer=1))

    for i, (b, g) in enumerate(arrivals):
        slot = rank - b
        how = dict(wait=1)
        if queue and queue[0] == (b, g):
            queue.pop(0)
            how["forward"] = 1
            while queue and queue[0][0] == rank:
                if "then" in how:
                    steps.append(pack(REST, slot, g, **how))
                    how = {}
                how["then"] = queue.pop(0)[1] + 1
        left[g] -= 1
        if g in waiting:
            waiting[g] -= 1
            if g in ready:
                steps.append(pack(NEXT, slot, g, answer=1, flag=KEEP if waiting[g] else RETURN, **how))
                how = {}
            seen[g].append(slot)
        ends = left[g] == 0 and not (rank == last and g < moved)
        if g in waiting and waiting[g] and i + 1 < len(arrivals) and arrivals[i + 1][1] == g:
            if how:
                steps.append(pack(REST, slot, g, **how))
            later.append(pack(NEXT, slot, g))
        else:
            steps += later
            steps.append(pack(NEXT, slot, g, flag=FINISH if ends else KEEP, **how))
            later = []
        for h in waiting:
            due = i + 1 < len(arrivals) and arrivals[i + 1][1] == h and waiting[h] == 1
            if h not in ready and (due or i >= taken_up(phase, h)):
                start_answer(h)
        if rank == last:
            while returned < moved and returns_before(order, moved, returned, groups) <= i + 1:
                steps.append(pack(MERGE, 0, returned))
                returned += 1
    if rank == last:
        steps += [pack(MERGE, 0, g) for g in range(returned, moved)]
    assert not queue and not later
    return before, steps, len(arrivals)


def returns_before(order, moved, g, groups):
    at = max(i for i, (_, h) in enumerate(order) if h == g)
    return groups - moved + sum(1 for _, h in order[:at] if h >= moved)


def scheduled_kernel(
    n, groups, per_group, most,
    q_hbm, k_hbm, v_hbm, o,
    q, qt, kv, m, l, acc, back, back_stats, mine, mine_stats,
    load_sem, send_sem, aside_sem, recv_sem, stats_sem,
):
    rows = kv.shape[2] // 2
    tall = per_group * HEAD_SIZE
    wide = per_group * rows
    me = lax.axis_index("seq")
    phase = lax.rem(lax.axis_index("batch"), 2)
    last, helper = n - 1, n - 2

    def kv_load(g):
        cols = pl.ds(g * HEAD_SIZE, HEAD_SIZE)
        return (
            pltpu.make_async_copy(
                k_hbm.at[0, :, cols], kv.at[0, g, pl.ds(0, rows)], load_sem.at[0]
            ),
            pltpu.make_async_copy(
                v_hbm.at[0, :, cols], kv.at[0, g, pl.ds(rows, rows)], load_sem.at[0]
            ),
        )

    def q_load(g):
        cols = pl.ds(g * tall, tall)
        return pltpu.make_async_copy(q_hbm.at[0, :, cols], q.at[g], load_sem.at[1])

    scripts = {(r, p): script(n, groups, p, r) for r in range(n) for p in range(2)}
    here = {key: (me == key[0]) & (phase == key[1]) for key in scripts}

    def wait_for(ref, sem):
        pltpu.make_async_copy(ref, ref, sem).wait()

    def send(slot, g, nth):
        return pltpu.make_async_remote_copy(
            src_ref=kv.at[slot, g],
            dst_ref=kv.at[slot + 1, g],
            send_sem=send_sem.at[0],
            recv_sem=recv_sem.at[nth],
            device_id={"seq": jnp.minimum(me + 1, last)},
            device_id_type=MESH,
        )

    def arrived(ref, nth):
        pltpu.make_async_copy(ref, ref, recv_sem.at[nth]).wait()

    asked_at = scripts[helper, 0][2]
    given_at = jnp.where(phase == 0, scripts[last, 0][2], scripts[last, 1][2])

    def ask(g):
        return pltpu.make_async_remote_copy(
            src_ref=q.at[g],
            dst_ref=q.at[groups + g],
            send_sem=aside_sem.at[0],
            recv_sem=recv_sem.at[asked_at + g],
            device_id={"seq": jnp.int32(helper)},
            device_id_type=MESH,
        )

    def give(g):
        return (
            pltpu.make_async_remote_copy(
                src_ref=mine.at[g],
                dst_ref=back.at[g],
                send_sem=aside_sem.at[0],
                recv_sem=recv_sem.at[given_at + g],
                device_id={"seq": jnp.int32(last)},
                device_id_type=MESH,
            ),
            pltpu.make_async_remote_copy(
                src_ref=mine_stats.at[g],
                dst_ref=back_stats.at[g],
                send_sem=aside_sem.at[1],
                recv_sem=stats_sem.at[g],
                device_id={"seq": jnp.int32(last)},
                device_id_type=MESH,
            ),
        )

    barrier = pltpu.get_barrier_semaphore()

    @pl.when(me > 0)
    def _():
        pl.semaphore_signal(barrier, inc=1, device_id={"seq": me - 1}, device_id_type=MESH)

    if most:
        @pl.when(me == helper)
        def _():
            pl.semaphore_signal(barrier, inc=1, device_id={"seq": jnp.int32(last)}, device_id_type=MESH)

    for g in range(groups):
        for copy in kv_load(g):
            copy.start()
    for g in range(groups):
        q_load(g).start()

    def pick(values):
        out = jnp.int32(0)
        for key, value in values.items():
            if value:
                out = jnp.where(here[key], jnp.int32(value), out)
        return out

    count = pick({key: len(steps) for key, (_, steps, _) in scripts.items()})
    longest = max(len(steps) for _, steps, _ in scripts.values())
    words = []
    for at in range(0, longest, 2):
        pairs = {key: (steps[at : at + 2] + [0, 0])[:2] for key, (_, steps, _) in scripts.items()}
        words.append(pick({key: low + CODE * high for key, (low, high) in pairs.items()}))

    @pl.when(me < last if not most else me >= 0)
    def _():
        pl.semaphore_wait(barrier, 1)

    wait_for(kv.at[0], load_sem.at[0])

    for (rank, p), (before, _, _) in scripts.items():
        @pl.when(here[rank, p])
        def _(before=before):
            for i, g in enumerate(before):
                send(0, g, i).start()

    wait_for(q.at[pl.ds(0, groups)], load_sem.at[1])

    for p in range(2):
        for g in range(moved_heads(n, groups, p)):
            @pl.when(here[last, p])
            def _(g=g):
                ask(g).start()

    sent_before = pick({key: len(before) for key, (before, _, _) in scripts.items()})

    def scores_of(slot, g, turned):
        return jnp.dot(kv[slot, g, :rows, :], turned, preferred_element_type=jnp.float32)

    def weighted(p, slot, g):
        return jnp.dot(
            kv[slot, g, rows:, :].T, p.astype(jnp.bfloat16), preferred_element_type=jnp.float32
        )

    def write(total, g):
        done = total.astype(jnp.bfloat16)
        for h in range(per_group):
            at = pl.multiple_of((g * per_group + h) * HEAD_SIZE, HEAD_SIZE)
            o[0, :, pl.ds(at, HEAD_SIZE)] = done[:, h * rows : (h + 1) * rows].T

    def conclude(qi, g, flag):
        @pl.when(flag == FINISH)
        def _():
            write(acc[qi] * (1.0 / l[qi]), g)

        if most:
            @pl.when(flag == RETURN)
            def _():
                mine[g] = (acc[qi] * (1.0 / l[qi])).astype(jnp.bfloat16)
                mine_stats[g, 0:1] = m[qi]
                mine_stats[g, 1:2] = l[qi]
                for copy in give(g):
                    copy.start()

    key = lax.broadcasted_iota(jnp.int32, (rows, wide), 0)
    query = lax.rem(lax.broadcasted_iota(jnp.int32, (rows, wide), 1), rows)

    def step(i, counts):
        got, sent = counts
        at = jnp.maximum(i - groups, 0)
        word = words[0] if words else jnp.int32(0)
        for j, other in enumerate(words[1:]):
            word = jnp.where(at >= 2 * (j + 1), other, word)
        code = jnp.where(lax.rem(at, 2) == 0, lax.rem(word, CODE), lax.div(word, CODE))
        own = pack(FIRST, 0, 0) + jnp.where(me == 0, pack(FIRST, 0, 0, flag=FINISH), 0) + pack(FIRST, 0, 1) * i
        code = jnp.where(i < groups, own, code)
        op = lax.rem(code, 4)
        slot = lax.rem(lax.div(code, 4), 4)
        g = lax.rem(lax.div(code, 16), 4)
        answer = lax.rem(lax.div(code, 64), 2)
        wait = lax.rem(lax.div(code, 128), 2)
        forward = lax.rem(lax.div(code, 256), 2)
        then = lax.rem(lax.div(code, 512), 8)
        flag = lax.div(code, 4096)
        qi = g + groups * answer

        @pl.when(wait == 1)
        def _():
            arrived(kv.at[slot, g], got)

            @pl.when(forward == 1)
            def _():
                send(slot, g, sent).start()

        sent = sent + forward

        @pl.when(then > 0)
        def _():
            send(0, then - 1, sent).start()

        if most:
            @pl.when((op == FIRST) & (answer == 1))
            def _():
                arrived(q.at[groups + g], asked_at + g)

        @pl.when(op == FIRST)
        def _():
            for h in range(per_group):
                qt[qi, :, h * rows : (h + 1) * rows] = q[qi, :, h * HEAD_SIZE : (h + 1) * HEAD_SIZE].T
            s = jnp.where(key <= query + rows * answer, scores_of(0, g, qt[qi]), -1e30)
            new_m = jnp.max(s, axis=0, keepdims=True)
            p = jnp.exp2((s - new_m) * SCALE)
            m[qi] = new_m
            l[qi] = jnp.sum(p, axis=0, keepdims=True)
            acc[qi] = weighted(p, 0, g)
            conclude(qi, g, flag)

        @pl.when(op == NEXT)
        def _():
            s = scores_of(slot, g, qt[qi])
            old_m = m[qi]
            new_m = jnp.maximum(old_m, jnp.max(s, axis=0, keepdims=True))
            fade = jnp.exp2((old_m - new_m) * SCALE)
            p = jnp.exp2((s - new_m) * SCALE)
            m[qi] = new_m
            l[qi] = l[qi] * fade + jnp.sum(p, axis=0, keepdims=True)
            acc[qi] = acc[qi] * fade + weighted(p, slot, g)
            conclude(qi, g, flag)

        if most:
            @pl.when(op == MERGE)
            def _():
                arrived(back.at[g], given_at + g)
                wait_for(back_stats.at[g], stats_sem.at[g])
                here, there = m[g], back_stats[g, 0:1]
                new_m = jnp.maximum(here, there)
                fade = jnp.exp2((here - new_m) * SCALE)
                weight = jnp.exp2((there - new_m) * SCALE) * back_stats[g, 1:2]
                share = 1.0 / (l[g] * fade + weight)
                write(acc[g] * (fade * share) + back[g].astype(jnp.float32) * (weight * share), g)

        return got + wait, sent + jnp.where(then > 0, 1, 0)

    lax.fori_loop(0, groups + count, step, (jnp.int32(0), sent_before))

    for (rank, p) in scripts:
        away = moved_heads(n, groups, p)

        @pl.when(here[rank, p])
        def _(rank=rank, away=away):
            if rank < helper:
                wait_for(kv.at[pl.ds(0, rank + 1)], send_sem.at[0])
            elif rank == helper:
                wait_for(kv.at[pl.ds(0, rank + 1), pl.ds(away, groups - away)], send_sem.at[0])
                if away:
                    wait_for(mine.at[pl.ds(0, away)], aside_sem.at[0])
                    wait_for(mine_stats.at[pl.ds(0, away)], aside_sem.at[1])
            elif away:
                wait_for(q.at[pl.ds(0, away)], aside_sem.at[0])


def scheduled(n, queries, keys, values):
    rows, query_width = queries.shape[1:]
    groups = keys.shape[2] // HEAD_SIZE
    per_group = query_width // HEAD_SIZE // groups
    tall, wide = per_group * HEAD_SIZE, per_group * rows
    most = max(moved_heads(n, groups, p) for p in range(2))
    held = max(most, 1)
    hbm = pl.BlockSpec(memory_space=pltpu.HBM)
    total = groups + most
    received = max(
        script(n, groups, p, r)[2] + (moved_heads(n, groups, p) if r >= n - 2 else 0)
        for p in range(2)
        for r in range(n)
    )
    bytes_held = (
        2 * rows * query_width * 2
        + total * rows * tall * (2 + 2 + 4)
        + 2 * n * rows * keys.shape[2] * 2
        + 2 * held * rows * tall * 2
        + (2 * total + 4 * held) * 8 * wide * 4
    )
    return pl.pallas_call(
        functools.partial(scheduled_kernel, n, groups, per_group, most),
        out_shape=jax.ShapeDtypeStruct(queries.shape, queries.dtype),
        in_specs=[hbm, hbm, hbm],
        out_specs=pl.BlockSpec(memory_space=pltpu.VMEM),
        scratch_shapes=[
            pltpu.VMEM((total, rows, tall), jnp.bfloat16),
            pltpu.VMEM((total, HEAD_SIZE, wide), jnp.bfloat16),
            pltpu.VMEM((n, groups, 2 * rows, HEAD_SIZE), jnp.bfloat16),
            pltpu.VMEM((total, 1, wide), jnp.float32),
            pltpu.VMEM((total, 1, wide), jnp.float32),
            pltpu.VMEM((total, HEAD_SIZE, wide), jnp.float32),
            pltpu.VMEM((held, HEAD_SIZE, wide), jnp.bfloat16),
            pltpu.VMEM((held, 2, wide), jnp.float32),
            pltpu.VMEM((held, HEAD_SIZE, wide), jnp.bfloat16),
            pltpu.VMEM((held, 2, wide), jnp.float32),
            pltpu.SemaphoreType.DMA((2,)),
            pltpu.SemaphoreType.DMA((1,)),
            pltpu.SemaphoreType.DMA((2,)),
            pltpu.SemaphoreType.DMA((received,)),
            pltpu.SemaphoreType.DMA((held,)),
        ],
        compiler_params=pltpu.CompilerParams(
            collective_id=0, has_side_effects=True, vmem_limit_bytes=bytes_held + 4 * 2**20
        ),
    )(*(pltpu.with_memory_space_constraint(x, pltpu.HBM) for x in (queries, keys, values)))


def kernel(
    n, groups, per_group,
    q_hbm, k_hbm, v_hbm, o,
    q, kv, m, acc,
    load_sem, q_sem, send_sem, recv_sem,
):
    rows = q.shape[0]
    me = lax.axis_index("seq")
    right, left = lax.rem(me + 1, n), lax.rem(me + n - 1, n)

    def loads(g):
        cols = pl.ds(g * HEAD_SIZE, HEAD_SIZE)
        return (
            pltpu.make_async_copy(
                k_hbm.at[0, :, cols], kv.at[0, g, pl.ds(0, rows)], load_sem.at[0, g]
            ),
            pltpu.make_async_copy(
                v_hbm.at[0, :, cols], kv.at[0, g, pl.ds(rows, rows)], load_sem.at[1, g]
            ),
        )

    def send(slot, g):
        return pltpu.make_async_remote_copy(
            src_ref=kv.at[slot, g],
            dst_ref=kv.at[slot + 1, g],
            send_sem=send_sem.at[slot, g],
            recv_sem=recv_sem.at[slot + 1, g],
            device_id={"seq": right},
            device_id_type=MESH,
        )

    def receive(slot, g):
        return pltpu.make_async_remote_copy(
            src_ref=kv.at[slot, g],
            dst_ref=kv.at[slot, g],
            send_sem=send_sem.at[slot, g],
            recv_sem=recv_sem.at[slot, g],
            device_id={"seq": right},
            device_id_type=MESH,
        )

    q_copy = pltpu.make_async_copy(q_hbm.at[0], q, q_sem)

    barrier = pltpu.get_barrier_semaphore()

    @pl.when(me > 0)
    def _():
        pl.semaphore_signal(barrier, inc=1, device_id={"seq": left}, device_id_type=MESH)

    for g in range(groups):
        for copy in loads(g):
            copy.start()
    q_copy.start()

    @pl.when(me < n - 1)
    def _():
        pl.semaphore_wait(barrier, 1)

    for g in range(groups):
        for copy in loads(g):
            copy.wait()

        @pl.when(me < n - 1)
        def _():
            send(0, g).start()

    q_copy.wait()

    def scores_of(slot, g):
        stacked = jnp.concatenate(
            [
                q[:, (g * per_group + h) * HEAD_SIZE : (g * per_group + h + 1) * HEAD_SIZE]
                for h in range(per_group)
            ],
            axis=0,
        )
        return lax.dot_general(
            stacked,
            kv[slot, g, :rows, :],
            (((1,), (1,)), ((), ())),
            preferred_element_type=jnp.float32,
        )

    def weighted(p, slot, g):
        block = jnp.concatenate(
            [kv[slot, g, rows:, :], jnp.ones((rows, HEAD_SIZE), jnp.bfloat16)], axis=1
        )
        return jnp.dot(p.astype(jnp.bfloat16), block, preferred_element_type=jnp.float32)

    def finish(total, g):
        done = (total[:, :HEAD_SIZE] / total[:, HEAD_SIZE:]).astype(jnp.bfloat16)
        for h in range(per_group):
            at = (g * per_group + h) * HEAD_SIZE
            o[0, :, at : at + HEAD_SIZE] = done[h * rows : (h + 1) * rows]

    row = lax.rem(lax.broadcasted_iota(jnp.int32, (per_group * rows, rows), 0), rows)
    visible = lax.broadcasted_iota(jnp.int32, (per_group * rows, rows), 1) <= row

    for g in range(groups):
        s = jnp.where(visible, scores_of(0, g), -1e30)
        new_m = jnp.max(s, axis=1, keepdims=True)
        total = weighted(jnp.exp2((s - new_m) * SCALE), 0, g)
        acc[g] = total
        m[g] = jnp.broadcast_to(new_m, m.shape[1:])

        @pl.when(me == 0)
        def _():
            finish(acc[g], g)

    @pl.loop(1, me + 1)
    def _(slot):
        for g in range(groups):
            receive(slot, g).wait_recv()

            @pl.when(me < n - 1)
            def _():
                send(slot, g).start()

            s = scores_of(slot, g)
            old_m = m[g]
            new_m = jnp.maximum(old_m, jnp.max(s, axis=1, keepdims=True))
            fade = jnp.exp2((old_m - new_m) * SCALE)
            p = jnp.exp2((s - new_m[:, :1]) * SCALE)
            total = acc[g] * jnp.concatenate([fade, fade], axis=1) + weighted(p, slot, g)

            @pl.when(slot < me)
            def _():
                acc[g] = total
                m[g] = new_m

            @pl.when(slot == me)
            def _():
                finish(total, g)

    @pl.when(me < n - 1)
    def _():
        @pl.loop(0, me + 1)
        def _(slot):
            for g in range(groups):
                send(slot, g).wait_send()


def on_device(n, queries, keys, values):
    rows, query_width = queries.shape[1:]
    groups = keys.shape[2] // HEAD_SIZE
    per_group = query_width // HEAD_SIZE // groups
    hbm = pl.BlockSpec(memory_space=pltpu.HBM)
    held = (2 * rows * query_width + 2 * n * rows * keys.shape[2]) * 2 + 3 * rows * query_width * 4
    return pl.pallas_call(
        functools.partial(kernel, n, groups, per_group),
        out_shape=jax.ShapeDtypeStruct(queries.shape, queries.dtype),
        in_specs=[hbm, hbm, hbm],
        out_specs=pl.BlockSpec(memory_space=pltpu.VMEM),
        scratch_shapes=[
            pltpu.VMEM((rows, query_width), jnp.bfloat16),
            pltpu.VMEM((n, groups, 2 * rows, HEAD_SIZE), jnp.bfloat16),
            pltpu.VMEM((groups, per_group * rows, HEAD_SIZE), jnp.float32),
            pltpu.VMEM((groups, per_group * rows, 2 * HEAD_SIZE), jnp.float32),
            pltpu.SemaphoreType.DMA((2, groups)),
            pltpu.SemaphoreType.DMA,
            pltpu.SemaphoreType.DMA((n, groups)),
            pltpu.SemaphoreType.DMA((n, groups)),
        ],
        compiler_params=pltpu.CompilerParams(collective_id=0, has_side_effects=True, vmem_limit_bytes=held + 4 * 2**20),
    )(*(pltpu.with_memory_space_constraint(x, pltpu.HBM) for x in (queries, keys, values)))


def solution(mesh):
    spec = P(("groups", "batch"), "seq", None)
    n = mesh.shape["seq"]
    return jax.shard_map(
        functools.partial(scheduled if n <= SCHEDULED else on_device, n),
        mesh=mesh,
        in_specs=(spec, spec, spec),
        out_specs=spec,
        check_vma=False,
    )
```
